256 devices in a mesh: gx: 16 (over z, core), gy: 4 (over x), gz: 4 (over y).
Axes of the slice: x: 4, y: 4, z: 8, core: 2. Of those that a mesh axis runs over, the one named last changes fastest.
Arguments:
- quant_codes: int32 [512, 128, 512], P('gx', 'gy', 'gz'), may hold values from -1073741824 to 1073741824, as said below
- error_step: float32 [1], replicated, may hold values from 4e-09 to 1.5e-08
Outputs:
- decoded: float32 [512, 128, 512], P('gx', 'gy', 'gz')
The draws below stay inside these ranges and needn't reach their ends.
Inputs may be any that keep to these rules, and one draw needn't show every extreme that they name: quant_codes are the third differences (along the three dimensions, with zeros before the grid's first cells) of a field of integers between -134217728 and 134217728.
All inputs are finite; a program needn't handle non-finite values.
Results may differ from the reference program's by a relative error of at most 0.00002.
Values sent between devices are 32-bit elements; how exact they have to be, the bound alone decides.
No kernel may reach another device: no remote copies, remote signals or barrier semaphores. Data moves between devices by JAX's collectives and lax.ppermute only.
A program may use at most 64 MiB of HBM per device.

```python
import math
import jax
import jax.numpy as jnp

QMAX = 134217728
NX = 512
NY = 128
NZ = 512


def draw_quant_codes(key, part):
    levels_grid = jax.random.randint(jax.random.fold_in(key, 11), (NX, NY, NZ), -QMAX, QMAX + 1, dtype=jnp.int32)
    first = levels_grid - jnp.pad(levels_grid, ((1, 0), (0, 0), (0, 0)))[:-1]
    second = first - jnp.pad(first, ((0, 0), (1, 0), (0, 0)))[:, :-1]
    third = second - jnp.pad(second, ((0, 0), (0, 0), (1, 0)))[:, :, :-1]
    return third.astype(jnp.int32)


def setup_inputs(seed: int = 0) -> dict:
    streams_of = jax.random.split(jax.random.key(seed), 3)
    quant_codes = draw_quant_codes(jax.random.fold_in(streams_of[2], 71), 0)
    error_step = jnp.clip(jnp.exp(jax.random.uniform(streams_of[1], (1,), jnp.float32, math.log(3.999999886872274e-09), math.log(1.4999999464748726e-08))), 3.999999886872274e-09, 1.4999999464748726e-08)
    return {"quant_codes": quant_codes, "error_step": error_step}


def reference(quant_codes, error_step):
    prefix = jnp.cumsum(quant_codes, axis=0, dtype=jnp.int32)
    prefix = jnp.cumsum(prefix, axis=1, dtype=jnp.int32)
    prefix = jnp.cumsum(prefix, axis=2, dtype=jnp.int32)
    recon = prefix.astype(jnp.float32) * error_step[0]
    padded = jnp.pad(recon, 1)
    neighbours = padded[2:, 1:-1, 1:-1] + padded[:-2, 1:-1, 1:-1]
    neighbours = neighbours + padded[1:-1, 2:, 1:-1] + padded[1:-1, :-2, 1:-1]
    neighbours = neighbours + padded[1:-1, 1:-1, 2:] + padded[1:-1, 1:-1, :-2]
    return recon + 0.5 * (neighbours / 6.0 - recon)
```

```python
import functools

import jax
import jax.numpy as jnp
from jax import lax
from jax.experimental import pallas as pl
from jax.experimental.pallas import tpu as pltpu
from jax.sharding import PartitionSpec as P

I32 = jnp.int32
LIMIT = 16 * 1024 * 1024


def params():
    return pltpu.CompilerParams(vmem_limit_bytes=LIMIT)


def at_lane(tile, lane):
    return jnp.broadcast_to(tile[:, lane : lane + 1], tile.shape)


def scan_lanes(v, lane):
    s = 1
    while s < v.shape[1]:
        v = v + jnp.where(lane >= s, pltpu.roll(v, s, 1), 0)
        s *= 2
    return v


def scan_rows(v, row):
    for s in (1, 2, 4):
        v = v + jnp.where(row >= s, pltpu.roll(v, s, 0), 0)
    return v


def prefix_kernel(q, full, y_last, y_first, z_last, z_first, send, *, me, n):
    nx, ny, _ = q.shape
    tiles = ny // 8
    lane = lax.broadcasted_iota(I32, (8, 128), 1)
    row = lax.broadcasted_iota(I32, (8, 128), 0)
    zero = jnp.zeros((8, 128), I32)
    sums, zl, zf = [zero] * tiles, [zero] * tiles, [zero] * tiles
    for i in range(nx):
        carry = None
        for t in range(tiles):
            rows = slice(8 * t, 8 * t + 8)
            v = scan_rows(scan_lanes(q[i, rows, :], lane), row)
            if carry is not None:
                v = v + carry
            if t + 1 < tiles:
                carry = jnp.broadcast_to(v[7:8, :], v.shape)
            v = v + sums[t] if i else v
            if t + 1 < tiles:
                pass
            sums[t] = v
            full[i, rows, :] = v
            zl[t] = jnp.where(lane == i, at_lane(v, 127), zl[t])
            zf[t] = jnp.where(lane == i, at_lane(v, 0), zf[t])
        y_first[i : i + 1, :] = sums[0][0:1, :]
        y_last[i : i + 1, :] = sums[-1][7:8, :]
    for t in range(tiles):
        z_last[8 * t : 8 * t + 8, :] = zl[t]
        z_first[8 * t : 8 * t + 8, :] = zf[t]
    x = lax.axis_index(me)
    for d in range(n):
        for t in range(tiles):
            rows = slice(8 * t, 8 * t + 8)
            send[d, rows, :] = jnp.where(d == x - 1, full[0, rows, :], sums[t])


def faces_kernel(got, y_last, y_first, z_last, z_first, low, high, send, *, n, ny, nz):
    x, y, z = lax.axis_index("gx"), lax.axis_index("gy"), lax.axis_index("gz")
    lane = lax.broadcasted_iota(I32, (32, 128), 1)
    c = jnp.zeros((32, 128), I32)
    for s in range(n):
        c = c + jnp.where(s < x, got[s], 0)
    h = got[jnp.minimum(x + 1, n - 1)]
    low[...] = c
    high[...] = h
    yl, yf, zl, zf = y_last[...], y_first[...], z_last[...], z_first[...]
    yl_main = yl + c[31:32, :]
    yf_main = yf + c[0:1, :]
    below = c[31:32, :]
    above = yl[31:32, :] + c[31:32, :] + h[31:32, :]
    row = lax.broadcasted_iota(I32, (8, 128), 0)
    yl_tail = jnp.where(row == 0, below, jnp.where(row == 1, above, 0))
    zl_main = zl + at_lane(c, 127)
    zl_main = zl_main + jnp.where(lane == 33, at_lane(zl, 31) + at_lane(h, 127), 0)
    zf_main = zf + at_lane(c, 0)
    for a in range(ny):
        for b in range(nz):
            main = jnp.where(
                b == z,
                jnp.where(a > y, yl_main, yf_main),
                jnp.where(b > z, zl_main, zf_main),
            )
            send[a * nz + b, 0:32, :] = main
            send[a * nz + b, 32:40, :] = yl_tail


def stencil_kernel(step, got, full, low, high, out, *, n, ny, nz):
    x, y, z = lax.axis_index("gx"), lax.axis_index("gy"), lax.axis_index("gz")
    nx = full.shape[0]
    lane = lax.broadcasted_iota(I32, (32, 128), 1)
    row = lax.broadcasted_iota(I32, (32, 128), 0)
    ay = jnp.zeros((40, 128), I32)
    az = jnp.zeros((32, 128), I32)
    ayz = jnp.zeros((1, 128), I32)
    hyz = jnp.zeros((1, 128), I32)
    yp, zp = jnp.minimum(y + 1, ny - 1), jnp.minimum(z + 1, nz - 1)
    hz = got[y * nz + zp, 0:32, :]
    for a in range(ny - 1):
        ay = ay + jnp.where(a < y, got[a * nz + z], 0)
        hz = hz + jnp.where(a < y, got[a * nz + zp, 31:32, :], 0)
        for b in range(nz - 1):
            ayz = ayz + jnp.where((a < y) & (b < z), got[a * nz + b, 31:32, :], 0)
    for b in range(nz - 1):
        az = az + jnp.where(b < z, got[y * nz + b, 0:32, :], 0)
        hyz = hyz + jnp.where(b < z, got[yp * nz + b, 0:1, :], 0)
    az = az + ayz
    hy = got[yp * nz + z, 0:32, :]
    has_x = (x < n - 1).astype(jnp.float32)
    has_y = (y < ny - 1).astype(jnp.float32)
    has_z = (z < nz - 1).astype(jnp.float32)
    half = step[0] * 0.5
    twelfth = step[0] * (1.0 / 12.0)
    f32 = jnp.float32
    c = low[...]

    def plane(i):
        k = nx if i < 0 else nx + 1 if i == nx else i
        left = at_lane(az, k)
        here = c + left + ay[k : k + 1, :]
        if i >= 0:
            here = here + full[min(i, nx - 1)]
        if i == nx:
            here = here + high[...]
        return here, left

    before = plane(-1)[0].astype(f32)
    now, left = plane(0)
    now_f = now.astype(f32)
    for i in range(nx):
        after, after_left = plane(i + 1)
        after_f = after.astype(f32)
        if i == nx - 1:
            after_f = after_f * has_x
        total = before + after_f
        up = (ay[i : i + 1, :] + jnp.broadcast_to(ayz[:, i : i + 1], (1, 128))).astype(f32)
        down = now[31:32, :] + hy[i : i + 1, :] + jnp.broadcast_to(hyz[:, i : i + 1], (1, 128))
        down = down.astype(f32) * has_y
        total = total + jnp.where(row == 0, up, pltpu.roll(now_f, 1, 0))
        total = total + jnp.where(row == 31, down, pltpu.roll(now_f, 31, 0))
        right = (now + at_lane(hz, i)).astype(f32) * has_z
        total = total + jnp.where(lane == 0, left.astype(f32), pltpu.roll(now_f, 1, 1))
        total = total + jnp.where(lane == 127, right, pltpu.roll(now_f, 127, 1))
        out[i] = now_f * half + total * twelfth
        before, now, now_f, left = now_f, after, after_f, after_left


def on_device(quant_codes, error_step):
    n, ny, nz = (lax.axis_size(a) for a in ("gx", "gy", "gz"))
    face = jax.ShapeDtypeStruct((32, 128), I32)
    full, y_last, y_first, z_last, z_first, send = pl.pallas_call(
        functools.partial(prefix_kernel, me="gx", n=n),
        out_shape=(
            jax.ShapeDtypeStruct(quant_codes.shape, I32),
            face,
            face,
            face,
            face,
            jax.ShapeDtypeStruct((n, 32, 128), I32),
        ),
        compiler_params=params(),
        name="prefix",
    )(quant_codes)
    got = lax.all_to_all(send, "gx", split_axis=0, concat_axis=0, tiled=True)
    low, high, send = pl.pallas_call(
        functools.partial(faces_kernel, n=n, ny=ny, nz=nz),
        out_shape=(face, face, jax.ShapeDtypeStruct((ny * nz, 40, 128), I32)),
        compiler_params=params(),
        name="faces",
    )(got, y_last, y_first, z_last, z_first)
    got = lax.all_to_all(send, ("gy", "gz"), split_axis=0, concat_axis=0, tiled=True)
    vmem = pl.BlockSpec(memory_space=pltpu.VMEM)
    return pl.pallas_call(
        functools.partial(stencil_kernel, n=n, ny=ny, nz=nz),
        in_specs=[pl.BlockSpec(memory_space=pltpu.SMEM)] + [vmem] * 4,
        out_shape=jax.ShapeDtypeStruct(quant_codes.shape, jnp.float32),
        compiler_params=params(),
        name="stencil",
    )(error_step, got, full, low, high)


def solution(mesh):
    spec = P("gx", "gy", "gz")
    return jax.shard_map(
        on_device, mesh=mesh, in_specs=(spec, P()), out_specs=spec, check_vma=False
    )
```

```python
import functools

import jax
import jax.numpy as jnp
from jax import lax
from jax.experimental import pallas as pl
from jax.experimental.pallas import tpu as pltpu
from jax.sharding import PartitionSpec as P

I32 = jnp.int32
LIMIT = 16 * 1024 * 1024


def params():
    return pltpu.CompilerParams(vmem_limit_bytes=LIMIT)


def at_lane(tile, lane):
    return jnp.broadcast_to(tile[:, lane : lane + 1], tile.shape)


def prefix_planes(v):
    lane = lax.broadcasted_iota(I32, v.shape, 1)
    for s in (1, 2, 4, 8, 16, 32, 64):
        v = v + jnp.where(lane >= s, pltpu.roll(v, s, 1), 0)
    v = v.reshape(-1, 8, 128)
    row = lax.broadcasted_iota(I32, v.shape, 1)
    for s in (1, 2, 4):
        v = v + jnp.where(row >= s, pltpu.roll(v, s, 1), 0)
    v = v.reshape(-1, 4, 8, 128)
    tiles = [v[:, 0]]
    for t in range(1, 4):
        tiles.append(v[:, t] + tiles[-1][:, 7:8, :])
    return tiles


def planes_kernel(q, pair):
    total = q[0]
    for i in range(1, q.shape[0]):
        total = total + q[i]
    tiles = prefix_planes(jnp.concatenate([total, q[0]], 0))
    for t in range(4):
        for p in range(2):
            pair[32 * p + 8 * t : 32 * p + 8 * t + 8, :] = tiles[t][p]


def block_kernel(step, q, full, y_last, y_first, z_last, z_first, scale):
    nx = q.shape[0]
    lane = lax.broadcasted_iota(I32, (8, 128), 1)
    zero = jnp.zeros((8, 128), I32)
    sums, zl, zf = [zero] * 4, [zero] * 4, [zero] * 4
    for g in range(0, nx, 8):
        tiles = prefix_planes(q[g : g + 8].reshape(256, 128))
        for i in range(8):
            for t in range(4):
                sums[t] = sums[t] + tiles[t][i]
                full[g + i, 8 * t : 8 * t + 8, :] = sums[t]
                zl[t] = jnp.where(lane == g + i, at_lane(sums[t], 127), zl[t])
                zf[t] = jnp.where(lane == g + i, at_lane(sums[t], 0), zf[t])
            y_first[g + i : g + i + 1, :] = sums[0][0:1, :]
            y_last[g + i : g + i + 1, :] = sums[3][7:8, :]
    for t in range(4):
        z_last[8 * t : 8 * t + 8, :] = zl[t]
        z_first[8 * t : 8 * t + 8, :] = zf[t]
    scale[...] = jnp.full((8, 128), step[0], jnp.float32)


def pack_kernel(mine, other, send):
    x = lax.axis_index("gx")
    chip, south = x // 2, x % 2 == 0
    both = mine[0:32, :] + other[0:32, :]
    first = jnp.where(south, mine[32:64, :], other[32:64, :])
    for d in range(send.shape[0]):
        send[d] = jnp.where(d == chip - 1, first, both)


def faces_kernel(
    got, other, y_last, y_first, z_last, z_first, low, high, send, *, ny, nz
):
    x, y, z = lax.axis_index("gx"), lax.axis_index("gy"), lax.axis_index("gz")
    chips = got.shape[0]
    chip, south = x // 2, x % 2 == 0
    lane = lax.broadcasted_iota(I32, (32, 128), 1)
    c = jnp.where(south, 0, other[0:32, :])
    for s in range(chips - 1):
        c = c + jnp.where(s < chip, got[s], 0)
    h = jnp.where(south, other[32:64, :], got[jnp.minimum(chip + 1, chips - 1)])
    low[...] = c
    high[...] = h
    yl, yf, zl, zf = y_last[...], y_first[...], z_last[...], z_first[...]
    yl_main = yl + c[31:32, :]
    yf_main = yf + c[0:1, :]
    below = c[31:32, :]
    above = yl[31:32, :] + c[31:32, :] + h[31:32, :]
    row = lax.broadcasted_iota(I32, (8, 128), 0)
    yl_tail = jnp.where(row == 0, below, jnp.where(row == 1, above, 0))
    zl_main = zl + at_lane(c, 127)
    zl_main = zl_main + jnp.where(lane == 33, at_lane(zl, 31) + at_lane(h, 127), 0)
    zf_main = zf + at_lane(c, 0)
    for a in range(ny):
        for b in range(nz):
            main = jnp.where(
                b == z,
                jnp.where(a > y, yl_main, yf_main),
                jnp.where(b > z, zl_main, zf_main),
            )
            send[a * nz + b, 0:32, :] = main
            send[a * nz + b, 32:40, :] = yl_tail


def stencil_kernel(step, got, full, low, high, out, *, n, ny, nz):
    x, y, z = lax.axis_index("gx"), lax.axis_index("gy"), lax.axis_index("gz")
    nx = full.shape[0]
    lane = lax.broadcasted_iota(I32, (32, 128), 1)
    row = lax.broadcasted_iota(I32, (32, 128), 0)
    ay = jnp.zeros((40, 128), I32)
    az = jnp.zeros((32, 128), I32)
    ayz = jnp.zeros((1, 128), I32)
    hyz = jnp.zeros((1, 128), I32)
    yp, zp = jnp.minimum(y + 1, ny - 1), jnp.minimum(z + 1, nz - 1)
    hz = got[y * nz + zp, 0:32, :]
    for a in range(ny - 1):
        ay = ay + jnp.where(a < y, got[a * nz + z], 0)
        hz = hz + jnp.where(a < y, got[a * nz + zp, 31:32, :], 0)
        for b in range(nz - 1):
            ayz = ayz + jnp.where((a < y) & (b < z), got[a * nz + b, 31:32, :], 0)
    for b in range(nz - 1):
        az = az + jnp.where(b < z, got[y * nz + b, 0:32, :], 0)
        hyz = hyz + jnp.where(b < z, got[yp * nz + b, 0:1, :], 0)
    az = az + ayz
    hy = got[yp * nz + z, 0:32, :]
    has_x = (x < n - 1).astype(jnp.float32)
    has_y = (y < ny - 1).astype(jnp.float32)
    has_z = (z < nz - 1).astype(jnp.float32)
    half = jnp.broadcast_to(step[0:1, :], (32, 128)) * 0.5
    twelfth = jnp.broadcast_to(step[0:1, :], (32, 128)) * (1.0 / 12.0)
    f32 = jnp.float32
    c = low[...]

    def plane(i):
        k = nx if i < 0 else nx + 1 if i == nx else i
        left = at_lane(az, k)
        here = c + left + ay[k : k + 1, :]
        if i >= 0:
            here = here + full[min(i, nx - 1)]
        if i == nx:
            here = here + high[...]
        return here, left

    before = plane(-1)[0].astype(f32)
    now, left = plane(0)
    now_f = now.astype(f32)
    for i in range(nx):
        after, after_left = plane(i + 1)
        after_f = after.astype(f32)
        if i == nx - 1:
            after_f = after_f * has_x
        total = before + after_f
        up = (ay[i : i + 1, :] + jnp.broadcast_to(ayz[:, i : i + 1], (1, 128))).astype(f32)
        down = now[31:32, :] + hy[i : i + 1, :] + jnp.broadcast_to(hyz[:, i : i + 1], (1, 128))
        down = down.astype(f32) * has_y
        total = total + jnp.where(row == 0, up, pltpu.roll(now_f, 1, 0))
        total = total + jnp.where(row == 31, down, pltpu.roll(now_f, 31, 0))
        right = (now + at_lane(hz, i)).astype(f32) * has_z
        total = total + jnp.where(lane == 0, left.astype(f32), pltpu.roll(now_f, 1, 1))
        total = total + jnp.where(lane == 127, right, pltpu.roll(now_f, 127, 1))
        out[i] = now_f * half + total * twelfth
        before, now, now_f, left = now_f, after, after_f, after_left


def on_device(quant_codes, error_step):
    n, ny, nz = (lax.axis_size(a) for a in ("gx", "gy", "gz"))
    shape = jax.ShapeDtypeStruct
    face = shape((32, 128), I32)
    vmem = pl.BlockSpec(memory_space=pltpu.VMEM)
    smem = pl.BlockSpec(memory_space=pltpu.SMEM)
    mine = pl.pallas_call(
        planes_kernel,
        out_shape=shape((64, 128), I32),
        compiler_params=params(),
        name="planes",
    )(quant_codes)
    other = lax.ppermute(mine, "gx", [(i, i ^ 1) for i in range(n)])
    full, y_last, y_first, z_last, z_first, scale = pl.pallas_call(
        block_kernel,
        in_specs=[smem, vmem],
        out_shape=(shape(quant_codes.shape, I32), face, face, face, face, shape((8, 128), jnp.float32)),
        compiler_params=params(),
        cost_estimate=pl.CostEstimate(flops=4_000_000, bytes_accessed=1_100_000, transcendentals=0),
        name="block",
    )(error_step, quant_codes)
    send = pl.pallas_call(
        pack_kernel,
        out_shape=shape((n // 2, 32, 128), I32),
        compiler_params=params(),
        name="pack",
    )(mine, other)
    same_core = [list(range(k, n, 2)) for k in range(2)]
    got = lax.all_to_all(
        send, "gx", split_axis=0, concat_axis=0, tiled=True, axis_index_groups=same_core
    )
    low, high, send = pl.pallas_call(
        functools.partial(faces_kernel, ny=ny, nz=nz),
        out_shape=(face, face, shape((ny * nz, 40, 128), I32)),
        compiler_params=params(),
        name="faces",
    )(got, other, y_last, y_first, z_last, z_first)
    got = lax.all_to_all(send, ("gy", "gz"), split_axis=0, concat_axis=0, tiled=True)
    return pl.pallas_call(
        functools.partial(stencil_kernel, n=n, ny=ny, nz=nz),
        out_shape=shape(quant_codes.shape, jnp.float32),
        compiler_params=params(),
        name="stencil",
    )(scale, got, full, low, high)


def solution(mesh):
    spec = P("gx", "gy", "gz")
    return jax.shard_map(
        on_device, mesh=mesh, in_specs=(spec, P()), out_specs=spec, check_vma=False
    )
```

```python
import functools

import jax
import jax.numpy as jnp
from jax import lax
from jax.experimental import pallas as pl
from jax.experimental.pallas import tpu as pltpu
from jax.sharding import PartitionSpec as P

I32 = jnp.int32
LIMIT = 16 * 1024 * 1024


def params():
    return pltpu.CompilerParams(vmem_limit_bytes=LIMIT)


def at_lane(tile, lane):
    return jnp.broadcast_to(tile[:, lane : lane + 1], tile.shape)


def prefix_lanes(v):
    k = lax.broadcasted_iota(I32, (256, 128), 0)
    upto = (k & 127) <= lax.broadcasted_iota(I32, (256, 128), 1)
    ones = jnp.where(upto, jnp.where(k < 128, 1.0, 256.0), 0.0).astype(jnp.bfloat16)

    def halves(low, high):
        both = jnp.concatenate([low, high], 1).astype(jnp.float32).astype(jnp.bfloat16)
        return jnp.dot(both, ones, preferred_element_type=jnp.float32).astype(I32)

    small = halves(v & 255, (v >> 8) & 255)
    large = halves((v >> 16) & 255, v >> 24)
    return small + (large << 16)


def prefix_planes(v):
    v = prefix_lanes(v).reshape(-1, 8, 128)
    row = lax.broadcasted_iota(I32, v.shape, 1)
    for s in (1, 2, 4):
        v = v + jnp.where(row >= s, pltpu.roll(v, s, 1), 0)
    v = v.reshape(-1, 4, 8, 128)
    tiles = [v[:, 0]]
    for t in range(1, 4):
        tiles.append(v[:, t] + tiles[-1][:, 7:8, :])
    return tiles


def planes_kernel(q, pair):
    sums = [q[i] for i in range(4)]
    for i in range(4, q.shape[0]):
        sums[i % 4] = sums[i % 4] + q[i]
    total = (sums[0] + sums[1]) + (sums[2] + sums[3])
    tiles = prefix_planes(jnp.concatenate([total, q[0]], 0))
    for t in range(4):
        for p in range(2):
            pair[32 * p + 8 * t : 32 * p + 8 * t + 8, :] = tiles[t][p]


def block_kernel(step, q, full, y_last, y_first, z_last, z_first, scale):
    nx = q.shape[0]
    lane = lax.broadcasted_iota(I32, (8, 128), 1)
    zero = jnp.zeros((8, 128), I32)
    sums, zl, zf = [zero] * 4, [zero] * 4, [zero] * 4
    for g in range(0, nx, 8):
        tiles = prefix_planes(q[g : g + 8].reshape(256, 128))
        for i in range(8):
            for t in range(4):
                sums[t] = sums[t] + tiles[t][i]
                full[g + i, 8 * t : 8 * t + 8, :] = sums[t]
                zl[t] = jnp.where(lane == g + i, at_lane(sums[t], 127), zl[t])
                zf[t] = jnp.where(lane == g + i, at_lane(sums[t], 0), zf[t])
            y_first[g + i : g + i + 1, :] = sums[0][0:1, :]
            y_last[g + i : g + i + 1, :] = sums[3][7:8, :]
    for t in range(4):
        z_last[8 * t : 8 * t + 8, :] = zl[t]
        z_first[8 * t : 8 * t + 8, :] = zf[t]
    scale[...] = jnp.full((8, 128), step[0], jnp.float32)


def pack_kernel(mine, other, _, send):
    x = lax.axis_index("gx")
    chip, south = x // 2, x % 2 == 0
    both = mine[0:32, :] + other[0:32, :]
    first = jnp.where(south, mine[32:64, :], other[32:64, :])
    for d in range(send.shape[0]):
        send[d] = jnp.where(d == chip - 1, first, both)


def faces_kernel(
    got, other, y_last, y_first, z_last, z_first, low, high, send, *, ny, nz
):
    x, y, z = lax.axis_index("gx"), lax.axis_index("gy"), lax.axis_index("gz")
    chips = got.shape[0]
    chip, south = x // 2, x % 2 == 0
    lane = lax.broadcasted_iota(I32, (32, 128), 1)
    c = jnp.where(south, 0, other[0:32, :])
    for s in range(chips - 1):
        c = c + jnp.where(s < chip, got[s], 0)
    h = jnp.where(south, other[32:64, :], got[jnp.minimum(chip + 1, chips - 1)])
    low[...] = c
    high[...] = h
    yl, yf, zl, zf = y_last[...], y_first[...], z_last[...], z_first[...]
    yl_main = yl + c[31:32, :]
    yf_main = yf + c[0:1, :]
    below = c[31:32, :]
    above = yl[31:32, :] + c[31:32, :] + h[31:32, :]
    row = lax.broadcasted_iota(I32, (8, 128), 0)
    yl_tail = jnp.where(row == 0, below, jnp.where(row == 1, above, 0))
    zl_main = zl + at_lane(c, 127)
    zl_main = zl_main + jnp.where(lane == 33, at_lane(zl, 31) + at_lane(h, 127), 0)
    zf_main = zf + at_lane(c, 0)
    for a in range(ny):
        for b in range(nz):
            main = jnp.where(
                b == z,
                jnp.where(a > y, yl_main, yf_main),
                jnp.where(b > z, zl_main, zf_main),
            )
            send[a * nz + b, 0:32, :] = main
            send[a * nz + b, 32:40, :] = yl_tail


def stencil_kernel(
    step, got, full, low, high, result, field, left, right, out, sems, *, n, ny, nz
):
    x, y, z = lax.axis_index("gx"), lax.axis_index("gy"), lax.axis_index("gz")
    f32 = jnp.float32
    nx = full.shape[0]
    ay = jnp.zeros((40, 128), I32)
    az = jnp.zeros((32, 128), I32)
    ayz = jnp.zeros((1, 128), I32)
    hyz = jnp.zeros((1, 128), I32)
    yp, zp = jnp.minimum(y + 1, ny - 1), jnp.minimum(z + 1, nz - 1)
    hz = got[y * nz + zp, 0:32, :]
    for a in range(ny - 1):
        ay = ay + jnp.where(a < y, got[a * nz + z], 0)
        hz = hz + jnp.where(a < y, got[a * nz + zp, 31:32, :], 0)
        for b in range(nz - 1):
            ayz = ayz + jnp.where((a < y) & (b < z), got[a * nz + b, 31:32, :], 0)
    for b in range(nz - 1):
        az = az + jnp.where(b < z, got[y * nz + b, 0:32, :], 0)
        hyz = hyz + jnp.where(b < z, got[yp * nz + b, 0:1, :], 0)
    az = az + ayz
    hy = got[yp * nz + z, 0:32, :]
    has_x = (x < n - 1).astype(f32)
    has_y = (y < ny - 1).astype(f32)
    has_z = (z < nz - 1).astype(f32)
    half = jnp.broadcast_to(step[0:1, :], (32, 128)) * 0.5
    twelfth = jnp.broadcast_to(step[0:1, :], (32, 128)) * (1.0 / 12.0)
    c = low[...]
    for i in range(-1, nx + 1):
        k = nx if i < 0 else nx + 1 if i == nx else i
        edge = at_lane(az, k)
        here = c + edge + ay[k : k + 1, :]
        if i >= 0:
            here = here + full[min(i, nx - 1)]
        if i == nx:
            field[i + 1, 8:40, :] = (here + high[...]).astype(f32) * has_x
            continue
        field[i + 1, 8:40, :] = here.astype(f32)
        if i < 0:
            continue
        left[i] = edge.astype(f32)
        right[i] = (here + at_lane(hz, i)).astype(f32) * has_z
        up = ay[i : i + 1, :] + jnp.broadcast_to(ayz[:, i : i + 1], (1, 128))
        field[i + 1, 7:8, :] = up.astype(f32)
        down = here[31:32, :] + hy[i : i + 1, :] + jnp.broadcast_to(hyz[:, i : i + 1], (1, 128))
        field[i + 1, 40:41, :] = down.astype(f32) * has_y
    lane = lax.broadcasted_iota(I32, (32, 128), 1)
    copies = []
    for i in range(nx):
        now = field[i + 1, 8:40, :]
        total = field[i, 8:40, :] + field[i + 2, 8:40, :]
        total = total + (field[i + 1, 7:39, :] + field[i + 1, 9:41, :])
        total = total + jnp.where(lane == 0, left[i], pltpu.roll(now, 1, 1))
        total = total + jnp.where(lane == 127, right[i], pltpu.roll(now, 127, 1))
        out[i] = now * half + total * twelfth
        if i % 8 == 7:
            rows = slice(i - 7, i + 1)
            copies.append(pltpu.make_async_copy(out.at[rows], result.at[rows], sems.at[i // 8]))
            copies[-1].start()
    for c in copies:
        c.wait()


def on_device(quant_codes, error_step):
    n, ny, nz = (lax.axis_size(a) for a in ("gx", "gy", "gz"))
    shape = jax.ShapeDtypeStruct
    face = shape((32, 128), I32)
    vmem = pl.BlockSpec(memory_space=pltpu.VMEM)
    smem = pl.BlockSpec(memory_space=pltpu.SMEM)
    hbm = pl.BlockSpec(memory_space=pltpu.HBM)
    mine = pl.pallas_call(
        planes_kernel,
        out_shape=shape((64, 128), I32),
        compiler_params=params(),
        name="planes",
    )(quant_codes)
    other = lax.ppermute(mine, "gx", [(i, i ^ 1) for i in range(n)])
    full, y_last, y_first, z_last, z_first, scale = pl.pallas_call(
        block_kernel,
        in_specs=[smem, vmem],
        out_shape=(shape(quant_codes.shape, I32), face, face, face, face, shape((8, 128), jnp.float32)),
        compiler_params=params(),
        cost_estimate=pl.CostEstimate(flops=4_000_000, bytes_accessed=1_100_000, transcendentals=0),
        name="block",
    )(error_step, quant_codes)
    send = pl.pallas_call(
        pack_kernel,
        in_specs=[vmem, vmem, pl.BlockSpec(memory_space=pl.ANY)],
        out_shape=shape((n // 2, 32, 128), I32),
        compiler_params=params(),
        name="pack",
    )(mine, other, scale)
    same_core = [list(range(k, n, 2)) for k in range(2)]
    got = lax.all_to_all(
        send, "gx", split_axis=0, concat_axis=0, tiled=True, axis_index_groups=same_core
    )
    low, high, send = pl.pallas_call(
        functools.partial(faces_kernel, ny=ny, nz=nz),
        out_shape=(face, face, shape((ny * nz, 40, 128), I32)),
        compiler_params=params(),
        name="faces",
    )(got, other, y_last, y_first, z_last, z_first)
    got = lax.all_to_all(send, ("gy", "gz"), split_axis=0, concat_axis=0, tiled=True)
    return pl.pallas_call(
        functools.partial(stencil_kernel, n=n, ny=ny, nz=nz),
        out_specs=hbm,
        out_shape=shape(quant_codes.shape, jnp.float32),
        scratch_shapes=[
            pltpu.VMEM((34, 48, 128), jnp.float32),
            pltpu.VMEM(quant_codes.shape, jnp.float32),
            pltpu.VMEM(quant_codes.shape, jnp.float32),
            pltpu.VMEM(quant_codes.shape, jnp.float32),
            pltpu.SemaphoreType.DMA((4,)),
        ],
        compiler_params=params(),
        name="stencil",
    )(scale, got, full, low, high)


def solution(mesh):
    spec = P("gx", "gy", "gz")
    return jax.shard_map(
        on_device, mesh=mesh, in_specs=(spec, P()), out_specs=spec, check_vma=False
    )
```

```python
import functools

import jax
import jax.numpy as jnp
from jax import lax
from jax.experimental import pallas as pl
from jax.experimental.pallas import tpu as pltpu
from jax.sharding import PartitionSpec as P

I32 = jnp.int32
LIMIT = 16 * 1024 * 1024


def params():
    return pltpu.CompilerParams(vmem_limit_bytes=LIMIT)


def at_lane(tile, lane):
    return jnp.broadcast_to(tile[:, lane : lane + 1], tile.shape)


def prefix_lanes(v):
    k = lax.broadcasted_iota(I32, (256, 128), 0)
    upto = (k & 127) <= lax.broadcasted_iota(I32, (256, 128), 1)
    ones = jnp.where(upto, jnp.where(k < 128, 1.0, 256.0), 0.0).astype(jnp.bfloat16)

    def halves(low, high):
        both = jnp.concatenate([low, high], 1).astype(jnp.float32).astype(jnp.bfloat16)
        return jnp.dot(both, ones, preferred_element_type=jnp.float32).astype(I32)

    small = halves(v & 255, (v >> 8) & 255)
    large = halves((v >> 16) & 255, v >> 24)
    return small + (large << 16)


def prefix_planes(v):
    v = prefix_lanes(v).reshape(-1, 8, 128)
    row = lax.broadcasted_iota(I32, v.shape, 1)
    for s in (1, 2, 4):
        v = v + jnp.where(row >= s, pltpu.roll(v, s, 1), 0)
    v = v.reshape(-1, 4, 8, 128)
    tiles = [v[:, 0]]
    for t in range(1, 4):
        tiles.append(v[:, t] + tiles[-1][:, 7:8, :])
    return tiles


def planes_kernel(q, pair):
    sums = [q[i] for i in range(4)]
    for i in range(4, q.shape[0]):
        sums[i % 4] = sums[i % 4] + q[i]
    total = (sums[0] + sums[1]) + (sums[2] + sums[3])
    tiles = prefix_planes(jnp.concatenate([total, q[0]], 0))
    for t in range(4):
        for p in range(2):
            pair[32 * p + 8 * t : 32 * p + 8 * t + 8, :] = tiles[t][p]


def block_kernel(step, q, full, faces, scale):
    nx = q.shape[0]
    lane = lax.broadcasted_iota(I32, (8, 128), 1)
    zero = jnp.zeros((8, 128), I32)
    sums, zl, zf = [zero] * 4, [zero] * 4, [zero] * 4
    for g in range(0, nx, 8):
        tiles = prefix_planes(q[g : g + 8].reshape(256, 128))
        for i in range(8):
            for t in range(4):
                sums[t] = sums[t] + tiles[t][i]
                full[g + i, 8 * t : 8 * t + 8, :] = sums[t]
                zl[t] = jnp.where(lane == g + i, at_lane(sums[t], 127), zl[t])
                zf[t] = jnp.where(lane == g + i, at_lane(sums[t], 0), zf[t])
            faces[g + i : g + i + 1, :] = sums[3][7:8, :]
            faces[32 + g + i : 33 + g + i, :] = sums[0][0:1, :]
    for t in range(4):
        faces[64 + 8 * t : 72 + 8 * t, :] = zl[t]
        faces[96 + 8 * t : 104 + 8 * t, :] = zf[t]
    scale[...] = jnp.full((8, 128), step[0], jnp.float32)


def chip_kernel(mine, other, send):
    send[0:32, :] = mine[0:32, :] + other[0:32, :]
    send[32:64, :] = other[32:64, :]


def pair_kernel(sent, got, send, state):
    chip = lax.axis_index("gx") // 2
    odd = chip % 2 == 1
    send[0:32, :] = sent[0:32, :] + got[0:32, :]
    send[32:64, :] = got[32:64, :]
    state[0:32, :] = jnp.where(odd, got[0:32, :], 0)
    state[32:64, :] = got[32:64, :]


def quad_kernel(sent, got, before, send, state):
    chip = lax.axis_index("gx") // 2
    send[0:32, :] = sent[0:32, :] + got[0:32, :]
    send[32:64, :] = got[32:64, :]
    state[0:32, :] = before[0:32, :] + jnp.where(chip % 4 >= 2, got[0:32, :], 0)
    state[32:64, :] = jnp.where(chip % 4 == 1, got[32:64, :], before[32:64, :])


def faces_kernel(got, before, other, mine, theirs, y_up, y_back, z_base, planes):
    chip, y = lax.axis_index("gx") // 2, lax.axis_index("gy")
    lane = lax.broadcasted_iota(I32, (32, 128), 1)
    row = lax.broadcasted_iota(I32, (8, 128), 0)
    c = before[0:32, :] + jnp.where(chip >= 4, got[0:32, :], 0)
    nxt = jnp.where(chip == 3, got[32:64, :], before[32:64, :])
    d = c + other[0:32, :]
    planes[0:32, :] = c
    planes[32:64, :] = d
    planes[64:96, :] = nxt
    last = d[31:32, :] + mine[31:32, :] + nxt[31:32, :]
    tail = jnp.where(row == 0, c[31:32, :], jnp.where(row == 1, last, 0))
    south, north = theirs[0:32, :] + c[31:32, :], mine[0:32, :] + d[31:32, :]
    y_up[0:32, :] = south
    y_up[32:64, :] = north
    y_up[64:72, :] = tail
    y_back[0:32, :] = jnp.where(y == 0, south, theirs[32:64, :] + c[0:1, :])
    y_back[32:64, :] = jnp.where(y == 0, north, mine[32:64, :] + d[0:1, :])
    y_back[64:72, :] = tail
    for k, at in ((64, 127), (96, 0)):
        low, high = at_lane(c, at), at_lane(d, at)
        above = high + at_lane(mine[k : k + 32, :], 31) + at_lane(nxt, at)
        base = jnp.where(lane < 32, theirs[k : k + 32, :] + low, 0)
        base = jnp.where((lane >= 32) & (lane < 64), pltpu.roll(mine[k : k + 32, :], 32, 1) + high, base)
        base = jnp.where(lane == 64, low, jnp.where(lane == 65, above, base))
        z_base[k - 64 : k - 32, :] = base


def lower(index, got1, got2, got3):
    one = jnp.where(index >= 1, got1[...], 0)
    two = jnp.where(index >= 2, got2[...], 0)
    return one + two + jnp.where(index >= 3, got3[...], 0)


def columns_kernel(got1, got2, got3, z_base, rows, z_up, z_back):
    y, z = lax.axis_index("gy"), lax.axis_index("gz")
    ay = lower(y, got1, got2, got3)
    hy = jnp.where(y < 3, got3[...], 0)
    rows[0:72, :] = ay
    rows[72:144, :] = hy
    pad = jnp.zeros((56, 128), I32)
    ay_t = jnp.concatenate([ay, pad], 0).T
    hy_t = jnp.concatenate([hy, pad], 0).T
    row = lax.broadcasted_iota(I32, (8, 128), 0)
    end = ay_t[127:128, :]
    tail = jnp.where(row == 0, end, jnp.where(row == 1, hy_t[127:128, :], 0))
    up = z_base[0:32, :] + end
    z_up[0:32, :] = up
    z_up[32:40, :] = tail
    z_back[0:32, :] = jnp.where(z == 0, up, z_base[32:64, :] + ay_t[0:1, :])
    z_back[32:40, :] = tail


def split_kernel(got1, got2, got3, rows, planes, south, north):
    z = lax.axis_index("gz")
    az = lower(z, got1, got2, got3)
    hz = got3[0:32, :]
    lane = lax.broadcasted_iota(I32, (40, 128), 1)
    row = lax.broadcasted_iota(I32, (8, 128), 0)

    def tail(a, b):
        return jnp.where(row == 0, rows[a : a + 1, :], jnp.where(row == 1, rows[b : b + 1, :], 0))

    south[0:32, :] = rows[0:32, :]
    south[32:40, :] = tail(64, 32)
    edges = jnp.where(lane == 32, at_lane(az, 64), jnp.where(lane == 33, at_lane(az, 32), az))
    south[40:80, :] = edges
    south[80:112, :] = hz
    south[112:144, :] = rows[72:104, :]
    south[144:176, :] = planes[0:32, :]
    north[0:32, :] = rows[32:64, :]
    north[32:40, :] = tail(31, 65)
    north[40:80, :] = jnp.where(lane == 32, at_lane(az, 31), pltpu.roll(az, 96, 1))
    north[80:112, :] = pltpu.roll(hz, 96, 1)
    north[112:144, :] = rows[104:136, :]
    north[144:176, :] = planes[32:64, :]


def stencil(step, pack, full, high, result, field, left, right, out, sems, *, n, ny, nz):
    x, y, z = lax.axis_index("gx"), lax.axis_index("gy"), lax.axis_index("gz")
    f32 = jnp.float32
    nx = full.shape[0]
    ay, az, hz, hy = pack[0:40, :], pack[40:72, :], pack[80:112, :], pack[112:144, :]
    ayz, hyz, c = pack[72:73, :], pack[73:74, :], pack[144:176, :]
    has_x = (x < n - 1).astype(f32)
    has_y = (y < ny - 1).astype(f32)
    has_z = (z < nz - 1).astype(f32)
    half = jnp.broadcast_to(step[0:1, :], (32, 128)) * 0.5
    twelfth = jnp.broadcast_to(step[0:1, :], (32, 128)) * (1.0 / 12.0)
    for i in range(-1, nx + 1):
        k = nx if i < 0 else nx + 1 if i == nx else i
        edge = at_lane(az, k)
        here = c + edge + ay[k : k + 1, :]
        if i >= 0:
            here = here + full[min(i, nx - 1)]
        if i == nx:
            field[i + 1, 8:40, :] = (here + high).astype(f32) * has_x
            continue
        field[i + 1, 8:40, :] = here.astype(f32)
        if i < 0:
            continue
        left[i] = edge.astype(f32)
        right[i] = (here + at_lane(hz, i)).astype(f32) * has_z
        up = ay[i : i + 1, :] + jnp.broadcast_to(ayz[:, i : i + 1], (1, 128))
        field[i + 1, 7:8, :] = up.astype(f32)
        down = here[31:32, :] + hy[i : i + 1, :] + jnp.broadcast_to(hyz[:, i : i + 1], (1, 128))
        field[i + 1, 40:41, :] = down.astype(f32) * has_y
    lane = lax.broadcasted_iota(I32, (32, 128), 1)
    copies = []
    for i in range(nx):
        now = field[i + 1, 8:40, :]
        total = field[i, 8:40, :] + field[i + 2, 8:40, :]
        total = total + (field[i + 1, 7:39, :] + field[i + 1, 9:41, :])
        total = total + jnp.where(lane == 0, left[i], pltpu.roll(now, 1, 1))
        total = total + jnp.where(lane == 127, right[i], pltpu.roll(now, 127, 1))
        out[i] = now * half + total * twelfth
        if i % 8 == 7:
            rows = slice(i - 7, i + 1)
            copies.append(pltpu.make_async_copy(out.at[rows], result.at[rows], sems.at[i // 8]))
            copies[-1].start()
    for c in copies:
        c.wait()


def north_kernel(step, pack, full, planes, *rest, **sizes):
    @pl.when(lax.axis_index("gx") % 2 == 1)
    def _():
        stencil(step, pack, full, planes[64:96, :], *rest, **sizes)


def south_kernel(step, pack, full, other, _, *rest, **sizes):
    @pl.when(lax.axis_index("gx") % 2 == 0)
    def _():
        stencil(step, pack, full, other[32:64, :], *rest, **sizes)


def routes(n, ny, nz):
    def route(move):
        pairs = []
        for x in range(n):
            for y in range(ny):
                for z in range(nz):
                    to = move(x, y, z) if x % 2 else (x, y ^ 1, z)
                    pairs.append(((x * ny + y) * nz + z, (to[0] * ny + to[1]) * nz + to[2]))
        return pairs

    across = [route(lambda x, y, z, d=d: (x ^ 2 * d, y, z)) for d in (1, 2, 4)]
    along_y = [route(lambda x, y, z, d=d: (x, (y + d) % ny, z)) for d in (1, 2, 3)]
    along_z = [route(lambda x, y, z, d=d: (x, y, (z + d) % nz)) for d in (1, 2, 3)]
    return across, along_y, along_z


def on_device(quant_codes, error_step):
    n, ny, nz = (lax.axis_size(a) for a in ("gx", "gy", "gz"))
    shape = jax.ShapeDtypeStruct
    vmem = pl.BlockSpec(memory_space=pltpu.VMEM)
    smem = pl.BlockSpec(memory_space=pltpu.SMEM)
    hbm = pl.BlockSpec(memory_space=pltpu.HBM)
    across, along_y, along_z = routes(n, ny, nz)

    def call(kernel, rows, *operands, **options):
        outs = tuple(shape((r, 128), I32) for r in rows)
        return pl.pallas_call(
            kernel, out_shape=outs, compiler_params=params(), name=kernel.__name__, **options
        )(*operands)

    def send(block, route):
        return lax.ppermute(block, ("gx", "gy", "gz"), route)

    def swap(block):
        return lax.ppermute(block, "gx", [(i, i ^ 1) for i in range(n)])

    (mine,) = call(planes_kernel, (64,), quant_codes)
    other = swap(mine)
    full, faces, scale = pl.pallas_call(
        block_kernel,
        in_specs=[smem, vmem],
        out_shape=(
            shape(quant_codes.shape, I32),
            shape((128, 128), I32),
            shape((8, 128), jnp.float32),
        ),
        compiler_params=params(),
        cost_estimate=pl.CostEstimate(flops=4_000_000, bytes_accessed=1_100_000, transcendentals=0),
        name="block",
    )(error_step, quant_codes)
    their_faces = swap(faces)
    (sent,) = call(chip_kernel, (64,), mine, other)
    got = send(sent, across[0])
    sent, state = call(pair_kernel, (64, 64), sent, got)
    got = send(sent, across[1])
    sent, state = call(quad_kernel, (64, 64), sent, got, state)
    got = send(sent, across[2])
    y_up, y_back, z_base, planes = call(
        faces_kernel, (72, 72, 64, 96), got, state, other, faces, their_faces
    )
    got = [send(b, r) for b, r in zip((y_up, y_up, y_back), along_y)]
    rows, z_up, z_back = call(columns_kernel, (144, 40, 40), *got, z_base)
    got = [send(b, r) for b, r in zip((z_up, z_up, z_back), along_z)]
    south, north = call(split_kernel, (176, 176), *got, rows, planes)
    pack = swap(south)
    sizes = dict(n=n, ny=ny, nz=nz)
    options = dict(
        out_specs=hbm,
        out_shape=shape(quant_codes.shape, jnp.float32),
        scratch_shapes=[
            pltpu.VMEM((34, 48, 128), jnp.float32),
            pltpu.VMEM(quant_codes.shape, jnp.float32),
            pltpu.VMEM(quant_codes.shape, jnp.float32),
            pltpu.VMEM(quant_codes.shape, jnp.float32),
            pltpu.SemaphoreType.DMA((4,)),
        ],
        compiler_params=params(),
        cost_estimate=pl.CostEstimate(flops=4_000_000, bytes_accessed=1_100_000, transcendentals=0),
    )
    result = pl.pallas_call(
        functools.partial(north_kernel, **sizes), in_specs=[vmem] * 4, name="north", **options
    )(scale, north, full, planes)
    return pl.pallas_call(
        functools.partial(south_kernel, **sizes),
        in_specs=[vmem] * 4 + [hbm],
        input_output_aliases={4: 0},
        name="south",
        **options,
    )(scale, pack, full, other, result)


def solution(mesh):
    spec = P("gx", "gy", "gz")
    return jax.shard_map(
        on_device, mesh=mesh, in_specs=(spec, P()), out_specs=spec, check_vma=False
    )
```

```python
import functools

import jax
import jax.numpy as jnp
from jax import lax
from jax.experimental import pallas as pl
from jax.experimental.pallas import tpu as pltpu
from jax.sharding import PartitionSpec as P


I32 = jnp.int32
LIMIT = 16 * 1024 * 1024


def params():
    return pltpu.CompilerParams(vmem_limit_bytes=LIMIT)


def at_lane(tile, lane):
    return jnp.broadcast_to(tile[:, lane : lane + 1], tile.shape)


def prefix_lanes(v):
    k = lax.broadcasted_iota(I32, (256, 128), 0)
    upto = (k & 127) <= lax.broadcasted_iota(I32, (256, 128), 1)
    ones = jnp.where(upto, jnp.where(k < 128, 1.0, 256.0), 0.0).astype(jnp.bfloat16)

    def halves(low, high):
        both = jnp.concatenate([low, high], 1).astype(jnp.float32).astype(jnp.bfloat16)
        return jnp.dot(both, ones, preferred_element_type=jnp.float32).astype(I32)

    small = halves(v & 255, (v >> 8) & 255)
    large = halves((v >> 16) & 255, v >> 24)
    return small + (large << 16)


def prefix_planes(v):
    v = prefix_lanes(v).reshape(-1, 8, 128)
    row = lax.broadcasted_iota(I32, v.shape, 1)
    for s in (1, 2, 4):
        v = v + jnp.where(row >= s, pltpu.roll(v, s, 1), 0)
    v = v.reshape(-1, 4, 8, 128)
    tiles = [v[:, 0]]
    for t in range(1, 4):
        tiles.append(v[:, t] + tiles[-1][:, 7:8, :])
    return tiles


def planes_kernel(q, pair):
    sums = [q[i] for i in range(4)]
    for i in range(4, q.shape[0]):
        sums[i % 4] = sums[i % 4] + q[i]
    total = (sums[0] + sums[1]) + (sums[2] + sums[3])
    tiles = prefix_planes(jnp.concatenate([total, q[0]], 0))
    for t in range(4):
        for p in range(2):
            pair[32 * p + 8 * t : 32 * p + 8 * t + 8, :] = tiles[t][p]


def block_kernel(step, q, full, faces, scale):
    nx = q.shape[0]
    lane = lax.broadcasted_iota(I32, (8, 128), 1)
    zero = jnp.zeros((8, 128), I32)
    sums, zl, zf = [zero] * 4, [zero] * 4, [zero] * 4
    for g in range(0, nx, 8):
        tiles = prefix_planes(q[g : g + 8].reshape(256, 128))
        for i in range(8):
            for t in range(4):
                sums[t] = sums[t] + tiles[t][i]
                full[g + i, 8 * t : 8 * t + 8, :] = sums[t]
                zl[t] = jnp.where(lane == g + i, at_lane(sums[t], 127), zl[t])
                zf[t] = jnp.where(lane == g + i, at_lane(sums[t], 0), zf[t])
            faces[g + i : g + i + 1, :] = sums[3][7:8, :]
            faces[32 + g + i : 33 + g + i, :] = sums[0][0:1, :]
    for t in range(4):
        faces[64 + 8 * t : 72 + 8 * t, :] = zl[t]
        faces[96 + 8 * t : 104 + 8 * t, :] = zf[t]
    scale[...] = jnp.full((8, 128), step[0], jnp.float32)


def chip_kernel(mine, other, send):
    send[0:32, :] = mine[0:32, :] + other[0:32, :]
    send[32:64, :] = other[32:64, :]


def pair_kernel(sent, got, _, send, state):
    chip = lax.axis_index("gx") // 2
    odd = chip % 2 == 1
    send[0:32, :] = sent[0:32, :] + got[0:32, :]
    send[32:64, :] = got[32:64, :]
    state[0:32, :] = jnp.where(odd, got[0:32, :], 0)
    state[32:64, :] = got[32:64, :]


def quad_kernel(sent, got, before, other, send, state):
    chip = lax.axis_index("gx") // 2
    send[0:32, :] = sent[0:32, :] + got[0:32, :]
    send[32:64, :] = other[32:64, :]
    state[0:32, :] = before[0:32, :] + jnp.where(chip % 4 >= 2, got[0:32, :], 0)
    state[32:64, :] = jnp.where(chip % 4 == 1, got[32:64, :], before[32:64, :])


def faces_kernel(got, before, other, mine, theirs, up, near, mid, z_base, planes):
    chip, y = lax.axis_index("gx") // 2, lax.axis_index("gy")
    lane = lax.broadcasted_iota(I32, (32, 128), 1)
    row = lax.broadcasted_iota(I32, (8, 128), 0)
    c = before[0:32, :] + jnp.where(chip >= 4, got[0:32, :], 0)
    nxt = jnp.where(chip == 3, got[32:64, :], before[32:64, :])
    d = c + other[0:32, :]
    planes[0:32, :] = c
    planes[32:64, :] = d
    planes[64:96, :] = nxt
    last = d[31:32, :] + mine[31:32, :] + nxt[31:32, :]
    tail = jnp.where(row == 0, c[31:32, :], jnp.where(row == 1, last, 0))
    halves = (theirs, c), (mine, d)
    for k, (face, plane) in enumerate(halves):
        rows = slice(32 * k, 32 * k + 32)
        last_row = face[0:32, :] + plane[31:32, :]
        first_row = face[32:64, :] + plane[0:1, :]
        up[rows, :] = last_row
        near[rows, :] = jnp.where(y % 2 == 1, first_row, last_row)
        mid[rows, :] = jnp.where(y == 2, first_row, last_row)
    for ref in (up, near, mid):
        ref[64:72, :] = tail
    for k, at in ((64, 127), (96, 0)):
        low, high = at_lane(c, at), at_lane(d, at)
        above = high + at_lane(mine[k : k + 32, :], 31) + at_lane(nxt, at)
        base = jnp.where(lane < 32, theirs[k : k + 32, :] + low, 0)
        base = jnp.where((lane >= 32) & (lane < 64), pltpu.roll(mine[k : k + 32, :], 32, 1) + high, base)
        base = jnp.where(lane == 64, low, jnp.where(lane == 65, above, base))
        z_base[k - 64 : k - 32, :] = base


def lower(index, got1, got2, got3):
    one = jnp.where(index % 2 == 1, got1[...], 0)
    two = jnp.where(index >= 2, got2[...], 0)
    return one + two + jnp.where(index >= 2, got3[...], 0)


def beyond(index, got1, got3):
    return jnp.where(index % 2 == 0, got1[...], got3[...])


def columns_kernel(got1, got2, got3, z_base, rows, up, near, mid):
    y, z = lax.axis_index("gy"), lax.axis_index("gz")
    ay = lower(y, got1, got2, got3)
    hy = jnp.where(y < 3, beyond(y, got1, got3), 0)
    rows[0:72, :] = ay
    rows[72:144, :] = hy
    pad = jnp.zeros((56, 128), I32)
    ay_t = jnp.concatenate([ay, pad], 0).T
    hy_t = jnp.concatenate([hy, pad], 0).T
    row = lax.broadcasted_iota(I32, (8, 128), 0)
    end = ay_t[127:128, :]
    tail = jnp.where(row == 0, end, jnp.where(row == 1, hy_t[127:128, :], 0))
    last = z_base[0:32, :] + end
    first = z_base[32:64, :] + ay_t[0:1, :]
    up[0:32, :] = last
    near[0:32, :] = jnp.where(z % 2 == 1, first, last)
    mid[0:32, :] = jnp.where(z == 2, first, last)
    for ref in (up, near, mid):
        ref[32:40, :] = tail


def split_kernel(got1, got2, got3, rows, planes, south, north):
    z = lax.axis_index("gz")
    az = lower(z, got1, got2, got3)
    hz = beyond(z, got1, got3)[0:32, :]
    lane = lax.broadcasted_iota(I32, (40, 128), 1)
    row = lax.broadcasted_iota(I32, (8, 128), 0)

    def tail(a, b):
        return jnp.where(row == 0, rows[a : a + 1, :], jnp.where(row == 1, rows[b : b + 1, :], 0))

    south[0:32, :] = rows[0:32, :]
    south[32:40, :] = tail(64, 32)
    edges = jnp.where(lane == 32, at_lane(az, 64), jnp.where(lane == 33, at_lane(az, 32), az))
    south[40:80, :] = edges
    south[80:112, :] = hz
    south[112:144, :] = rows[72:104, :]
    south[144:176, :] = planes[0:32, :]
    north[0:32, :] = rows[32:64, :]
    north[32:40, :] = tail(31, 65)
    north[40:80, :] = jnp.where(lane == 32, at_lane(az, 31), pltpu.roll(az, 96, 1))
    north[80:112, :] = pltpu.roll(hz, 96, 1)
    north[112:144, :] = rows[104:136, :]
    north[144:176, :] = planes[32:64, :]


def stencil(step, pack, full, high, result, field, left, right, out, sems, *, n, ny, nz):
    x, y, z = lax.axis_index("gx"), lax.axis_index("gy"), lax.axis_index("gz")
    f32 = jnp.float32
    nx = full.shape[0]
    ay, az, hz, hy = pack[0:40, :], pack[40:72, :], pack[80:112, :], pack[112:144, :]
    ayz, hyz, c = pack[72:73, :], pack[73:74, :], pack[144:176, :]
    has_x = (x < n - 1).astype(f32)
    has_y = (y < ny - 1).astype(f32)
    has_z = (z < nz - 1).astype(f32)
    half = jnp.broadcast_to(step[0:1, :], (32, 128)) * 0.5
    twelfth = jnp.broadcast_to(step[0:1, :], (32, 128)) * (1.0 / 12.0)
    for i in range(-1, nx + 1):
        k = nx if i < 0 else nx + 1 if i == nx else i
        edge = at_lane(az, k)
        here = c + edge + ay[k : k + 1, :]
        if i >= 0:
            here = here + full[min(i, nx - 1)]
        if i == nx:
            field[i + 1, 8:40, :] = (here + high).astype(f32) * has_x
            continue
        field[i + 1, 8:40, :] = here.astype(f32)
        if i < 0:
            continue
        left[i] = edge.astype(f32)
        right[i] = (here + at_lane(hz, i)).astype(f32) * has_z
        up = ay[i : i + 1, :] + jnp.broadcast_to(ayz[:, i : i + 1], (1, 128))
        field[i + 1, 7:8, :] = up.astype(f32)
        down = here[31:32, :] + hy[i : i + 1, :] + jnp.broadcast_to(hyz[:, i : i + 1], (1, 128))
        field[i + 1, 40:41, :] = down.astype(f32) * has_y
    lane = lax.broadcasted_iota(I32, (32, 128), 1)
    copies = []
    for i in range(nx):
        now = field[i + 1, 8:40, :]
        total = field[i, 8:40, :] + field[i + 2, 8:40, :]
        total = total + (field[i + 1, 7:39, :] + field[i + 1, 9:41, :])
        total = total + jnp.where(lane == 0, left[i], pltpu.roll(now, 1, 1))
        total = total + jnp.where(lane == 127, right[i], pltpu.roll(now, 127, 1))
        out[i] = now * half + total * twelfth
        if i % 8 == 7:
            rows = slice(i - 7, i + 1)
            copies.append(pltpu.make_async_copy(out.at[rows], result.at[rows], sems.at[i // 8]))
            copies[-1].start()
    for c in copies:
        c.wait()


def north_kernel(step, pack, full, planes, *rest, **sizes):
    @pl.when(lax.axis_index("gx") % 2 == 1)
    def _():
        stencil(step, pack, full, planes[64:96, :], *rest, **sizes)


def south_kernel(step, pack, full, other, _, *rest, **sizes):
    @pl.when(lax.axis_index("gx") % 2 == 0)
    def _():
        stencil(step, pack, full, other[32:64, :], *rest, **sizes)


def routes(n, ny, nz):
    def route(move):
        pairs = []
        for x in range(n):
            for y in range(ny):
                for z in range(nz):
                    to = move(x, y, z) if x % 2 else (x, y ^ 1, z)
                    pairs.append(((x * ny + y) * nz + z, (to[0] * ny + to[1]) * nz + to[2]))
        return pairs

    across = [route(lambda x, y, z, d=d: (x ^ d, y, z)) for d in (2, 4)]
    across.append(route(lambda x, y, z: (n - x, y, z)))
    along_y = [route(lambda x, y, z, d=d: (x, y ^ d, z)) for d in (1, 2, 3)]
    along_z = [route(lambda x, y, z, d=d: (x, y, z ^ d)) for d in (1, 2, 3)]
    return across, along_y, along_z


def on_device(quant_codes, error_step):
    n, ny, nz = (lax.axis_size(a) for a in ("gx", "gy", "gz"))
    shape = jax.ShapeDtypeStruct
    vmem = pl.BlockSpec(memory_space=pltpu.VMEM)
    smem = pl.BlockSpec(memory_space=pltpu.SMEM)
    hbm = pl.BlockSpec(memory_space=pltpu.HBM)
    across, along_y, along_z = routes(n, ny, nz)

    def call(kernel, rows, *operands, **options):
        outs = tuple(shape((r, 128), I32) for r in rows)
        return pl.pallas_call(
            kernel, out_shape=outs, compiler_params=params(), **options
        )(*operands)

    def send(block, route):
        return lax.ppermute(block, ("gx", "gy", "gz"), route)

    def exchange(blocks, routes):
        up, near, mid = blocks
        got = []
        for block, route in zip((near, up, mid), routes):
            got.append(send(block, route))
        return got

    def swap(block):
        return lax.ppermute(block, "gx", [(i, i ^ 1) for i in range(n)])

    (mine,) = call(planes_kernel, (64,), quant_codes)
    other = swap(mine)
    full, faces, scale = pl.pallas_call(
        block_kernel,
        in_specs=[smem, vmem],
        out_shape=(
            shape(quant_codes.shape, I32),
            shape((128, 128), I32),
            shape((8, 128), jnp.float32),
        ),
        compiler_params=params(),
        cost_estimate=pl.CostEstimate(flops=4_000_000, bytes_accessed=1_100_000, transcendentals=0),
        name="block",
    )(error_step, quant_codes)
    (sent,) = call(chip_kernel, (64,), mine, other)
    got = send(sent, across[0])
    sent, state = call(pair_kernel, (64, 64), sent, got, scale)
    got = send(sent, across[1])
    sent, state = call(quad_kernel, (64, 64), sent, got, state, other)
    their_faces = swap(faces)
    got = send(sent, across[2])
    *sent, z_base, planes = call(
        faces_kernel, (72, 72, 72, 64, 96), got, state, other, faces, their_faces
    )
    got = exchange(sent, along_y)
    rows, *sent = call(columns_kernel, (144, 40, 40, 40), *got, z_base)
    got = exchange(sent, along_z)
    south, north = call(split_kernel, (176, 176), *got, rows, planes)
    pack = swap(south)
    sizes = dict(n=n, ny=ny, nz=nz)
    options = dict(
        out_specs=hbm,
        out_shape=shape(quant_codes.shape, jnp.float32),
        scratch_shapes=[
            pltpu.VMEM((34, 48, 128), jnp.float32),
            pltpu.VMEM(quant_codes.shape, jnp.float32),
            pltpu.VMEM(quant_codes.shape, jnp.float32),
            pltpu.VMEM(quant_codes.shape, jnp.float32),
            pltpu.SemaphoreType.DMA((4,)),
        ],
        compiler_params=params(),
        cost_estimate=pl.CostEstimate(flops=4_000_000, bytes_accessed=1_100_000, transcendentals=0),
    )
    result = pl.pallas_call(
        functools.partial(north_kernel, **sizes), in_specs=[vmem] * 4, name="north", **options
    )(scale, north, full, planes)
    return pl.pallas_call(
        functools.partial(south_kernel, **sizes),
        in_specs=[vmem] * 4 + [hbm],
        input_output_aliases={4: 0},
        name="south",
        **options,
    )(scale, pack, full, other, result)


def solution(mesh):
    spec = P("gx", "gy", "gz")
    return jax.shard_map(
        on_device, mesh=mesh, in_specs=(spec, P()), out_specs=spec, check_vma=False
    )
```

```python
import functools

import jax
import jax.numpy as jnp
from jax import lax
from jax.experimental import pallas as pl
from jax.experimental.pallas import tpu as pltpu
from jax.sharding import PartitionSpec as P


I32 = jnp.int32
LIMIT = 16 * 1024 * 1024


def params():
    return pltpu.CompilerParams(vmem_limit_bytes=LIMIT)


def at_lane(tile, lane):
    return jnp.broadcast_to(tile[:, lane : lane + 1], tile.shape)


def prefix_lanes(v):
    k = lax.broadcasted_iota(I32, (256, 128), 0)
    upto = (k & 127) <= lax.broadcasted_iota(I32, (256, 128), 1)
    ones = jnp.where(upto, jnp.where(k < 128, 1.0, 256.0), 0.0).astype(jnp.bfloat16)

    def halves(low, high):
        both = jnp.concatenate([low, high], 1).astype(jnp.float32).astype(jnp.bfloat16)
        return jnp.dot(both, ones, preferred_element_type=jnp.float32).astype(I32)

    small = halves(v & 255, (v >> 8) & 255)
    large = halves((v >> 16) & 255, v >> 24)
    return small + (large << 16)


def prefix_planes(v):
    v = prefix_lanes(v).reshape(-1, 8, 128)
    row = lax.broadcasted_iota(I32, v.shape, 1)
    for s in (1, 2, 4):
        v = v + jnp.where(row >= s, pltpu.roll(v, s, 1), 0)
    v = v.reshape(-1, 4, 8, 128)
    tiles = [v[:, 0]]
    for t in range(1, 4):
        tiles.append(v[:, t] + tiles[-1][:, 7:8, :])
    return tiles


def planes_kernel(q, pair):
    sums = [q[i] for i in range(4)]
    for i in range(4, q.shape[0]):
        sums[i % 4] = sums[i % 4] + q[i]
    total = (sums[0] + sums[1]) + (sums[2] + sums[3])
    tiles = prefix_planes(jnp.concatenate([total, q[0]], 0))
    for t in range(4):
        for p in range(2):
            pair[32 * p + 8 * t : 32 * p + 8 * t + 8, :] = tiles[t][p]


def block_kernel(step, q, full, faces, scale):
    nx = q.shape[0]
    lane = lax.broadcasted_iota(I32, (8, 128), 1)
    zero = jnp.zeros((8, 128), I32)
    sums, zl, zf = [zero] * 4, [zero] * 4, [zero] * 4
    for g in range(0, nx, 8):
        tiles = prefix_planes(q[g : g + 8].reshape(256, 128))
        for i in range(8):
            for t in range(4):
                sums[t] = sums[t] + tiles[t][i]
                full[g + i, 8 * t : 8 * t + 8, :] = sums[t]
                zl[t] = jnp.where(lane == g + i, at_lane(sums[t], 127), zl[t])
                zf[t] = jnp.where(lane == g + i, at_lane(sums[t], 0), zf[t])
            faces[g + i : g + i + 1, :] = sums[3][7:8, :]
            faces[32 + g + i : 33 + g + i, :] = sums[0][0:1, :]
    for t in range(4):
        faces[64 + 8 * t : 72 + 8 * t, :] = zl[t]
        faces[96 + 8 * t : 104 + 8 * t, :] = zf[t]
    scale[...] = jnp.full((8, 128), step[0], jnp.float32)


def chip_kernel(mine, other, send):
    send[0:32, :] = mine[0:32, :] + other[0:32, :]
    send[32:64, :] = other[32:64, :]


def pair_kernel(sent, got, _, send, state):
    chip = lax.axis_index("gx") // 2
    odd = chip % 2 == 1
    send[0:32, :] = sent[0:32, :] + got[0:32, :]
    send[32:64, :] = got[32:64, :]
    state[0:32, :] = jnp.where(odd, got[0:32, :], 0)
    state[32:64, :] = got[32:64, :]


def quad_kernel(sent, got, before, other, _, send, state):
    chip = lax.axis_index("gx") // 2
    send[0:32, :] = sent[0:32, :] + got[0:32, :]
    send[32:64, :] = other[32:64, :]
    state[0:32, :] = before[0:32, :] + jnp.where(chip % 4 >= 2, got[0:32, :], 0)
    state[32:64, :] = jnp.where(chip % 4 == 1, got[32:64, :], before[32:64, :])


def faces_kernel(got, before, other, mine, theirs, up, near, mid, z_base, planes):
    chip, y = lax.axis_index("gx") // 2, lax.axis_index("gy")
    lane = lax.broadcasted_iota(I32, (32, 128), 1)
    row = lax.broadcasted_iota(I32, (8, 128), 0)
    c = before[0:32, :] + jnp.where(chip >= 4, got[0:32, :], 0)
    nxt = jnp.where(chip == 3, got[32:64, :], before[32:64, :])
    d = c + other[0:32, :]
    planes[0:32, :] = c
    planes[32:64, :] = d
    planes[64:96, :] = nxt
    last = d[31:32, :] + mine[31:32, :] + nxt[31:32, :]
    tail = jnp.where(row == 0, c[31:32, :], jnp.where(row == 1, last, 0))
    halves = (theirs, c), (mine, d)
    for k, (face, plane) in enumerate(halves):
        rows = slice(32 * k, 32 * k + 32)
        last_row = face[0:32, :] + plane[31:32, :]
        first_row = face[32:64, :] + plane[0:1, :]
        up[rows, :] = last_row
        near[rows, :] = jnp.where(y % 2 == 1, first_row, last_row)
        mid[rows, :] = jnp.where(y == 2, first_row, last_row)
    for ref in (up, near, mid):
        ref[64:72, :] = tail
    for k, at in ((64, 127), (96, 0)):
        low, high = at_lane(c, at), at_lane(d, at)
        above = high + at_lane(mine[k : k + 32, :], 31) + at_lane(nxt, at)
        base = jnp.where(lane < 32, theirs[k : k + 32, :] + low, 0)
        base = jnp.where((lane >= 32) & (lane < 64), pltpu.roll(mine[k : k + 32, :], 32, 1) + high, base)
        base = jnp.where(lane == 64, low, jnp.where(lane == 65, above, base))
        z_base[k - 64 : k - 32, :] = base


def lower(index, got1, got2, got3):
    one = jnp.where(index % 2 == 1, got1[...], 0)
    two = jnp.where(index >= 2, got2[...], 0)
    return one + two + jnp.where(index >= 2, got3[...], 0)


def beyond(index, got1, got3):
    return jnp.where(index % 2 == 0, got1[...], got3[...])


def columns_kernel(got1, got2, got3, z_base, rows, up, near, mid):
    y, z = lax.axis_index("gy"), lax.axis_index("gz")
    ay = lower(y, got1, got2, got3)
    hy = jnp.where(y < 3, beyond(y, got1, got3), 0)
    rows[0:72, :] = ay
    rows[72:144, :] = hy
    pad = jnp.zeros((56, 128), I32)
    ay_t = jnp.concatenate([ay, pad], 0).T
    hy_t = jnp.concatenate([hy, pad], 0).T
    row = lax.broadcasted_iota(I32, (8, 128), 0)
    end = ay_t[127:128, :]
    tail = jnp.where(row == 0, end, jnp.where(row == 1, hy_t[127:128, :], 0))
    last = z_base[0:32, :] + end
    first = z_base[32:64, :] + ay_t[0:1, :]
    up[0:32, :] = last
    near[0:32, :] = jnp.where(z % 2 == 1, first, last)
    mid[0:32, :] = jnp.where(z == 2, first, last)
    for ref in (up, near, mid):
        ref[32:40, :] = tail


def split_kernel(got1, got2, got3, rows, planes, south, north):
    z = lax.axis_index("gz")
    az = lower(z, got1, got2, got3)
    hz = beyond(z, got1, got3)[0:32, :]
    lane = lax.broadcasted_iota(I32, (40, 128), 1)
    row = lax.broadcasted_iota(I32, (8, 128), 0)

    def tail(a, b):
        return jnp.where(row == 0, rows[a : a + 1, :], jnp.where(row == 1, rows[b : b + 1, :], 0))

    south[0:32, :] = rows[0:32, :]
    south[32:40, :] = tail(64, 32)
    edges = jnp.where(lane == 32, at_lane(az, 64), jnp.where(lane == 33, at_lane(az, 32), az))
    south[40:80, :] = edges
    south[80:112, :] = hz
    south[112:144, :] = rows[72:104, :]
    south[144:176, :] = planes[0:32, :]
    north[0:32, :] = rows[32:64, :]
    north[32:40, :] = tail(31, 65)
    north[40:80, :] = jnp.where(lane == 32, at_lane(az, 31), pltpu.roll(az, 96, 1))
    north[80:112, :] = pltpu.roll(hz, 96, 1)
    north[112:144, :] = rows[104:136, :]
    north[144:176, :] = planes[32:64, :]


def inner_kernel(full, _, inner, field, *, ny, nz):
    has_y = lax.axis_index("gy") < ny - 1
    has_z = lax.axis_index("gz") < nz - 1
    nx = full.shape[0]
    lane = lax.broadcasted_iota(I32, (32, 128), 1)
    for i in range(nx):
        field[i, 8:40, :] = full[i]
        field[i, 7:8, :] = jnp.zeros((1, 128), I32)
        field[i, 40:41, :] = jnp.where(has_y, full[i, 31:32, :], 0)
    for i in range(nx):
        now = full[i]
        total = 6 * now + (field[i, 7:39, :] + field[i, 9:41, :])
        if i > 0:
            total = total + full[i - 1]
        if i < nx - 1:
            total = total + full[i + 1]
        total = total + jnp.where(lane == 0, 0, pltpu.roll(now, 1, 1))
        beyond_z = jnp.where(has_z, now, 0)
        inner[i] = total + jnp.where(lane == 127, beyond_z, pltpu.roll(now, 127, 1))


def stencil(step, pack, inner, full, high, result, out, sems, *, n, ny, nz):
    has_x = lax.axis_index("gx") < n - 1
    has_y = lax.axis_index("gy") < ny - 1
    has_z = lax.axis_index("gz") < nz - 1
    nx = full.shape[0]
    lane = lax.broadcasted_iota(I32, (32, 128), 1)
    row = lax.broadcasted_iota(I32, (32, 128), 0)
    ay, az, hz, hy = pack[0:32, :], pack[40:72, :], pack[80:112, :], pack[112:144, :]
    hyz, low = pack[73:74, :], pack[144:176, :]

    def beside(v, before, after, axis, last):
        at = lane if axis else row
        down = jnp.where(at == 0, before, pltpu.roll(v, 1, axis))
        return down + jnp.where(at == last, after, pltpu.roll(v, (-1) % v.shape[axis], axis))

    def held(flag, v):
        return jnp.where(flag, v, 0)

    rows = 8 * ay + beside(ay, pack[32:33, :], held(has_x, pack[33:34, :]), 0, 31)
    rows = rows + beside(ay, 0, held(has_z, ay), 1, 127)
    cols = 8 * az + beside(az, at_lane(az, 32), held(has_x, at_lane(az, 33)), 1, 31)
    cols = cols + beside(az, pack[72:73, :], held(has_y, az), 0, 31)
    both = 8 * low + beside(low, 0, held(has_y, low), 0, 31)
    both = both + beside(low, 0, held(has_z, low), 1, 127)
    end_y = jnp.where(has_y, hy, -ay)
    hyz = held(has_y, hyz)
    end_z = jnp.where(has_z, hz, -az)
    scale = jnp.broadcast_to(step[0:1, :], (32, 128)) * (1.0 / 12.0)
    copies = []
    for i in range(nx):
        total = inner[i] + (both + rows[i : i + 1, :]) + at_lane(cols, i)
        total = total + jnp.where(lane == 127, at_lane(end_z, i), 0)
        edge = end_y[i : i + 1, :] + jnp.broadcast_to(hyz[:, i : i + 1], (1, 128))
        total = total + jnp.where(row == 31, edge, 0)
        if i == nx - 1:
            total = total + jnp.where(has_x, full[i] + high, -low)
        out[i] = total.astype(jnp.float32) * scale
        if i % 8 == 7:
            part = slice(i - 7, i + 1)
            copies.append(pltpu.make_async_copy(out.at[part], result.at[part], sems.at[i // 8]))
            copies[-1].start()
    for c in copies:
        c.wait()


def north_kernel(step, pack, inner, full, planes, *rest, **sizes):
    @pl.when(lax.axis_index("gx") % 2 == 1)
    def _():
        stencil(step, pack, inner, full, planes[64:96, :], *rest, **sizes)


def south_kernel(step, pack, inner, full, other, _, *rest, **sizes):
    @pl.when(lax.axis_index("gx") % 2 == 0)
    def _():
        stencil(step, pack, inner, full, other[32:64, :], *rest, **sizes)


def routes(n, ny, nz):
    def route(move, south=lambda x, y, z: (x, y ^ 1, z)):
        pairs = []
        for x in range(n):
            for y in range(ny):
                for z in range(nz):
                    to = (move if x % 2 else south)(x, y, z)
                    pairs.append(((x * ny + y) * nz + z, (to[0] * ny + to[1]) * nz + to[2]))
        return pairs

    across = [route(lambda x, y, z, d=d: (x ^ d, y, z)) for d in (2, 4)]
    across.append(route(lambda x, y, z: (n - x, y, z)))
    along_y = [route(lambda x, y, z, d=d: (x, y ^ d, z)) for d in (1, 2)]
    along_z = [route(lambda x, y, z, d=d: (x, y, z ^ d)) for d in (1, 2)]

    def far(x, at, size):
        if x % 2:
            return (x, size - 1 - at) if at < size - 1 else (x - 1, at)
        return (x, at - 1) if at else (x + 1, at)

    def far_y(x, y, z):
        x, y = far(x, y, ny)
        return x, y, z

    def far_z(x, y, z):
        x, z = far(x, z, nz)
        return x, y, z

    along_y.append(route(far_y, far_y))
    along_z.append(route(far_z, far_z))
    return across, along_y, along_z


def on_device(quant_codes, error_step):
    n, ny, nz = (lax.axis_size(a) for a in ("gx", "gy", "gz"))
    shape = jax.ShapeDtypeStruct
    vmem = pl.BlockSpec(memory_space=pltpu.VMEM)
    smem = pl.BlockSpec(memory_space=pltpu.SMEM)
    hbm = pl.BlockSpec(memory_space=pltpu.HBM)
    across, along_y, along_z = routes(n, ny, nz)

    def call(kernel, rows, *operands, **options):
        outs = tuple(shape((r, 128), I32) for r in rows)
        return pl.pallas_call(
            kernel, out_shape=outs, compiler_params=params(), **options
        )(*operands)

    def send(block, route):
        return lax.ppermute(block, ("gx", "gy", "gz"), route)

    def exchange(blocks, routes):
        up, near, mid = blocks
        got = []
        for block, route in zip((near, up, mid), routes):
            got.append(send(block, route))
        return got

    def swap(block):
        return lax.ppermute(block, "gx", [(i, i ^ 1) for i in range(n)])

    (mine,) = call(planes_kernel, (64,), quant_codes)
    other = swap(mine)
    full, faces, scale = pl.pallas_call(
        block_kernel,
        in_specs=[smem, vmem],
        out_shape=(
            shape(quant_codes.shape, I32),
            shape((128, 128), I32),
            shape((8, 128), jnp.float32),
        ),
        compiler_params=params(),
        cost_estimate=pl.CostEstimate(flops=4_000_000, bytes_accessed=1_100_000, transcendentals=0),
        name="block",
    )(error_step, quant_codes)
    (sent,) = call(chip_kernel, (64,), mine, other)
    got = send(sent, across[0])
    sent, state = call(pair_kernel, (64, 64), sent, got, scale)
    got = send(sent, across[1])
    inner = pl.pallas_call(
        functools.partial(inner_kernel, ny=ny, nz=nz),
        out_shape=shape(quant_codes.shape, I32),
        scratch_shapes=[pltpu.VMEM((32, 48, 128), I32)],
        compiler_params=params(),
        cost_estimate=pl.CostEstimate(flops=4_000_000, bytes_accessed=1_100_000, transcendentals=0),
        name="inner",
    )(full, state)
    sent, state = call(quad_kernel, (64, 64), sent, got, state, other, inner)
    their_faces = swap(faces)
    got = send(sent, across[2])
    *sent, z_base, planes = call(
        faces_kernel, (72, 72, 72, 64, 96), got, state, other, faces, their_faces
    )
    got = exchange(sent, along_y)
    rows, *sent = call(columns_kernel, (144, 40, 40, 40), *got, z_base)
    got = exchange(sent, along_z)
    south, north = call(split_kernel, (176, 176), *got, rows, planes)
    pack = swap(south)
    sizes = dict(n=n, ny=ny, nz=nz)
    options = dict(
        out_specs=hbm,
        out_shape=shape(quant_codes.shape, jnp.float32),
        scratch_shapes=[
            pltpu.VMEM(quant_codes.shape, jnp.float32),
            pltpu.SemaphoreType.DMA((4,)),
        ],
        compiler_params=params(),
        cost_estimate=pl.CostEstimate(flops=4_000_000, bytes_accessed=1_100_000, transcendentals=0),
    )
    result = pl.pallas_call(
        functools.partial(north_kernel, **sizes), in_specs=[vmem] * 5, name="north", **options
    )(scale, north, inner, full, planes)
    return pl.pallas_call(
        functools.partial(south_kernel, **sizes),
        in_specs=[vmem] * 5 + [hbm],
        input_output_aliases={5: 0},
        name="south",
        **options,
    )(scale, pack, inner, full, other, result)


def solution(mesh):
    spec = P("gx", "gy", "gz")
    return jax.shard_map(
        on_device, mesh=mesh, in_specs=(spec, P()), out_specs=spec, check_vma=False
    )
```

```python
import functools

import jax
import jax.numpy as jnp
from jax import lax
from jax.experimental import pallas as pl
from jax.experimental.pallas import tpu as pltpu
from jax.sharding import PartitionSpec as P


I32 = jnp.int32
LIMIT = 16 * 1024 * 1024


def params():
    return pltpu.CompilerParams(vmem_limit_bytes=LIMIT)


def at_lane(tile, lane):
    return jnp.broadcast_to(tile[:, lane : lane + 1], tile.shape)


def prefix_lanes(v):
    k = lax.broadcasted_iota(I32, (256, 128), 0)
    upto = (k & 127) <= lax.broadcasted_iota(I32, (256, 128), 1)
    ones = jnp.where(upto, jnp.where(k < 128, 1.0, 256.0), 0.0).astype(jnp.bfloat16)

    def halves(low, high):
        both = jnp.concatenate([low, high], 1).astype(jnp.float32).astype(jnp.bfloat16)
        return jnp.dot(both, ones, preferred_element_type=jnp.float32).astype(I32)

    small = halves(v & 255, (v >> 8) & 255)
    large = halves((v >> 16) & 255, v >> 24)
    return small + (large << 16)


def prefix_planes(v):
    v = prefix_lanes(v).reshape(-1, 8, 128)
    row = lax.broadcasted_iota(I32, v.shape, 1)
    for s in (1, 2, 4):
        v = v + jnp.where(row >= s, pltpu.roll(v, s, 1), 0)
    v = v.reshape(-1, 4, 8, 128)
    tiles = [v[:, 0]]
    for t in range(1, 4):
        tiles.append(v[:, t] + tiles[-1][:, 7:8, :])
    return tiles


def planes_kernel(q, pair):
    sums = [q[i] for i in range(4)]
    for i in range(4, q.shape[0]):
        sums[i % 4] = sums[i % 4] + q[i]
    total = (sums[0] + sums[1]) + (sums[2] + sums[3])
    tiles = prefix_planes(jnp.concatenate([total, q[0]], 0))
    for t in range(4):
        for p in range(2):
            pair[32 * p + 8 * t : 32 * p + 8 * t + 8, :] = tiles[t][p]


def block_kernel(step, q, full, faces, scale):
    nx = q.shape[0]
    lane = lax.broadcasted_iota(I32, (8, 128), 1)
    zero = jnp.zeros((8, 128), I32)
    sums, zl, zf = [zero] * 4, [zero] * 4, [zero] * 4
    for g in range(0, nx, 8):
        tiles = prefix_planes(q[g : g + 8].reshape(256, 128))
        for i in range(8):
            for t in range(4):
                sums[t] = sums[t] + tiles[t][i]
                full[g + i, 8 * t : 8 * t + 8, :] = sums[t]
                zl[t] = jnp.where(lane == g + i, at_lane(sums[t], 127), zl[t])
                zf[t] = jnp.where(lane == g + i, at_lane(sums[t], 0), zf[t])
            faces[g + i : g + i + 1, :] = sums[3][7:8, :]
            faces[32 + g + i : 33 + g + i, :] = sums[0][0:1, :]
    for t in range(4):
        faces[64 + 8 * t : 72 + 8 * t, :] = zl[t]
        faces[96 + 8 * t : 104 + 8 * t, :] = zf[t]
    scale[...] = jnp.full((8, 128), step[0], jnp.float32)


def chip_kernel(mine, other, send):
    send[0:32, :] = mine[0:32, :] + other[0:32, :]
    send[32:64, :] = other[32:64, :]


def pair_kernel(sent, got, _, send, state):
    chip = lax.axis_index("gx") // 2
    odd = chip % 2 == 1
    send[0:32, :] = sent[0:32, :] + got[0:32, :]
    send[32:64, :] = got[32:64, :]
    state[0:32, :] = jnp.where(odd, got[0:32, :], 0)
    state[32:64, :] = got[32:64, :]


def quad_kernel(sent, got, before, other, _, send, state):
    chip = lax.axis_index("gx") // 2
    send[...] = jnp.where(chip == 4, other[32:64, :], sent[0:32, :] + got[0:32, :])
    state[0:32, :] = before[0:32, :] + jnp.where(chip % 4 >= 2, got[0:32, :], 0)
    state[32:64, :] = jnp.where(chip % 4 == 1, got[32:64, :], before[32:64, :])


def faces_kernel(got, before, other, mine, theirs, up, near, mid, z_base, planes):
    chip, y = lax.axis_index("gx") // 2, lax.axis_index("gy")
    lane = lax.broadcasted_iota(I32, (32, 128), 1)
    row = lax.broadcasted_iota(I32, (8, 128), 0)
    c = before[0:32, :] + jnp.where(chip >= 4, got[...], 0)
    nxt = jnp.where(chip == 3, got[...], before[32:64, :])
    d = c + other[0:32, :]
    planes[0:32, :] = c
    planes[32:64, :] = d
    planes[64:96, :] = nxt
    last = d[31:32, :] + mine[31:32, :] + nxt[31:32, :]
    tail = jnp.where(row == 0, c[31:32, :], jnp.where(row == 1, last, 0))
    halves = (theirs, c), (mine, d)
    for k, (face, plane) in enumerate(halves):
        rows = slice(32 * k, 32 * k + 32)
        last_row = face[0:32, :] + plane[31:32, :]
        first_row = face[32:64, :] + plane[0:1, :]
        up[rows, :] = last_row
        near[rows, :] = jnp.where(y % 2 == 1, first_row, last_row)
        mid[rows, :] = jnp.where(y == 2, first_row, last_row)
    for ref in (up, near, mid):
        ref[64:72, :] = tail
    for k, at in ((64, 127), (96, 0)):
        low, high = at_lane(c, at), at_lane(d, at)
        above = high + at_lane(mine[k : k + 32, :], 31) + at_lane(nxt, at)
        base = jnp.where(lane < 32, theirs[k : k + 32, :] + low, 0)
        base = jnp.where((lane >= 32) & (lane < 64), pltpu.roll(mine[k : k + 32, :], 32, 1) + high, base)
        base = jnp.where(lane == 64, low, jnp.where(lane == 65, above, base))
        z_base[k - 64 : k - 32, :] = base


def lower(index, got1, got2, got3):
    one = jnp.where(index % 2 == 1, got1[...], 0)
    two = jnp.where(index >= 2, got2[...], 0)
    return one + two + jnp.where(index >= 2, got3[...], 0)


def beyond(index, got1, got3):
    return jnp.where(index % 2 == 0, got1[...], got3[...])


def columns_kernel(got1, got2, got3, z_base, rows, up, near, mid):
    y, z = lax.axis_index("gy"), lax.axis_index("gz")
    ay = lower(y, got1, got2, got3)
    hy = jnp.where(y < 3, beyond(y, got1, got3), 0)
    rows[0:72, :] = ay
    rows[72:144, :] = hy
    pad = jnp.zeros((56, 128), I32)
    ay_t = jnp.concatenate([ay, pad], 0).T
    hy_t = jnp.concatenate([hy, pad], 0).T
    row = lax.broadcasted_iota(I32, (8, 128), 0)
    end = ay_t[127:128, :]
    tail = jnp.where(row == 0, end, jnp.where(row == 1, hy_t[127:128, :], 0))
    last = z_base[0:32, :] + end
    first = z_base[32:64, :] + ay_t[0:1, :]
    up[0:32, :] = last
    near[0:32, :] = jnp.where(z % 2 == 1, first, last)
    mid[0:32, :] = jnp.where(z == 2, first, last)
    for ref in (up, near, mid):
        ref[32:40, :] = tail


def split_kernel(got1, got2, got3, rows, planes, south, north):
    z = lax.axis_index("gz")
    az = lower(z, got1, got2, got3)
    hz = beyond(z, got1, got3)[0:32, :]
    lane = lax.broadcasted_iota(I32, (40, 128), 1)
    row = lax.broadcasted_iota(I32, (8, 128), 0)

    def tail(a, b):
        return jnp.where(row == 0, rows[a : a + 1, :], jnp.where(row == 1, rows[b : b + 1, :], 0))

    south[0:32, :] = rows[0:32, :]
    south[32:40, :] = tail(64, 32)
    edges = jnp.where(lane == 32, at_lane(az, 64), jnp.where(lane == 33, at_lane(az, 32), az))
    south[40:80, :] = edges
    south[80:112, :] = hz
    south[112:144, :] = rows[72:104, :]
    south[144:176, :] = planes[0:32, :]
    north[0:32, :] = rows[32:64, :]
    north[32:40, :] = tail(31, 65)
    north[40:80, :] = jnp.where(lane == 32, at_lane(az, 31), pltpu.roll(az, 96, 1))
    north[80:112, :] = pltpu.roll(hz, 96, 1)
    north[112:144, :] = rows[104:136, :]
    north[144:176, :] = planes[32:64, :]


def inner_kernel(full, _, inner, field, *, ny, nz):
    has_y = lax.axis_index("gy") < ny - 1
    has_z = lax.axis_index("gz") < nz - 1
    nx = full.shape[0]
    lane = lax.broadcasted_iota(I32, (32, 128), 1)
    for i in range(nx):
        field[i, 8:40, :] = full[i]
        field[i, 7:8, :] = jnp.zeros((1, 128), I32)
        field[i, 40:41, :] = jnp.where(has_y, full[i, 31:32, :], 0)
    for i in range(nx):
        now = full[i]
        total = 6 * now + (field[i, 7:39, :] + field[i, 9:41, :])
        if i > 0:
            total = total + full[i - 1]
        if i < nx - 1:
            total = total + full[i + 1]
        total = total + jnp.where(lane == 0, 0, pltpu.roll(now, 1, 1))
        beyond_z = jnp.where(has_z, now, 0)
        inner[i] = total + jnp.where(lane == 127, beyond_z, pltpu.roll(now, 127, 1))


def stencil(step, pack, inner, full, high, result, out, sems, *, n, ny, nz):
    has_x = lax.axis_index("gx") < n - 1
    has_y = lax.axis_index("gy") < ny - 1
    has_z = lax.axis_index("gz") < nz - 1
    nx = full.shape[0]
    lane = lax.broadcasted_iota(I32, (32, 128), 1)
    row = lax.broadcasted_iota(I32, (32, 128), 0)
    ay, az, hz, hy = pack[0:32, :], pack[40:72, :], pack[80:112, :], pack[112:144, :]
    hyz, low = pack[73:74, :], pack[144:176, :]

    def beside(v, before, after, axis, last):
        at = lane if axis else row
        down = jnp.where(at == 0, before, pltpu.roll(v, 1, axis))
        return down + jnp.where(at == last, after, pltpu.roll(v, (-1) % v.shape[axis], axis))

    def held(flag, v):
        return jnp.where(flag, v, 0)

    rows = 8 * ay + beside(ay, pack[32:33, :], held(has_x, pack[33:34, :]), 0, 31)
    rows = rows + beside(ay, 0, held(has_z, ay), 1, 127)
    cols = 8 * az + beside(az, at_lane(az, 32), held(has_x, at_lane(az, 33)), 1, 31)
    cols = cols + beside(az, pack[72:73, :], held(has_y, az), 0, 31)
    both = 8 * low + beside(low, 0, held(has_y, low), 0, 31)
    both = both + beside(low, 0, held(has_z, low), 1, 127)
    end_y = jnp.where(has_y, hy, -ay)
    hyz = held(has_y, hyz)
    end_z = jnp.where(has_z, hz, -az)
    scale = jnp.broadcast_to(step[0:1, :], (32, 128)) * (1.0 / 12.0)
    copies = []
    for i in range(nx):
        total = inner[i] + (both + rows[i : i + 1, :]) + at_lane(cols, i)
        total = total + jnp.where(lane == 127, at_lane(end_z, i), 0)
        edge = end_y[i : i + 1, :] + jnp.broadcast_to(hyz[:, i : i + 1], (1, 128))
        total = total + jnp.where(row == 31, edge, 0)
        if i == nx - 1:
            total = total + jnp.where(has_x, full[i] + high, -low)
        out[i] = total.astype(jnp.float32) * scale
        if i % 8 == 7:
            part = slice(i - 7, i + 1)
            copies.append(pltpu.make_async_copy(out.at[part], result.at[part], sems.at[i // 8]))
            copies[-1].start()
    for c in copies:
        c.wait()


def north_kernel(step, pack, inner, full, planes, *rest, **sizes):
    @pl.when(lax.axis_index("gx") % 2 == 1)
    def _():
        stencil(step, pack, inner, full, planes[64:96, :], *rest, **sizes)


def south_kernel(step, pack, inner, full, other, _, *rest, **sizes):
    @pl.when(lax.axis_index("gx") % 2 == 0)
    def _():
        stencil(step, pack, inner, full, other[32:64, :], *rest, **sizes)


def routes(n, ny, nz):
    def route(move, south=lambda x, y, z: (x, y ^ 1, z)):
        pairs = []
        for x in range(n):
            for y in range(ny):
                for z in range(nz):
                    to = (move if x % 2 else south)(x, y, z)
                    pairs.append(((x * ny + y) * nz + z, (to[0] * ny + to[1]) * nz + to[2]))
        return pairs

    across = [route(lambda x, y, z, d=d: (x ^ d, y, z)) for d in (2, 4)]
    across.append(route(lambda x, y, z: (n - x, y, z)))

    def middle(x, at, size):
        half = size // 2
        if x % 2:
            return (x, at + half) if at < half else (x - 1, at)
        return (x + 1, at) if at < half else (x, size - 1 - at)

    def far(x, at, size):
        if x % 2:
            return (x, size - 1 - at) if at < size - 1 else (x - 1, at)
        return (x, at - 1) if at else (x + 1, at)

    def in_y(step):
        def move(x, y, z):
            x, y = step(x, y, ny)
            return x, y, z

        return route(move, move)

    def in_z(step):
        def move(x, y, z):
            x, z = step(x, z, nz)
            return x, y, z

        return route(move, move)

    near_y = route(lambda x, y, z: (x, y ^ 1, z))
    near_z = route(lambda x, y, z: (x, y, z ^ 1))
    along_y = [near_y, in_y(middle), in_y(far)]
    along_z = [near_z, in_z(middle), in_z(far)]
    return across, along_y, along_z


def on_device(quant_codes, error_step):
    n, ny, nz = (lax.axis_size(a) for a in ("gx", "gy", "gz"))
    shape = jax.ShapeDtypeStruct
    vmem = pl.BlockSpec(memory_space=pltpu.VMEM)
    smem = pl.BlockSpec(memory_space=pltpu.SMEM)
    hbm = pl.BlockSpec(memory_space=pltpu.HBM)
    across, along_y, along_z = routes(n, ny, nz)

    def call(kernel, rows, *operands, **options):
        outs = tuple(shape((r, 128), I32) for r in rows)
        return pl.pallas_call(
            kernel, out_shape=outs, compiler_params=params(), **options
        )(*operands)

    def send(block, route):
        return lax.ppermute(block, ("gx", "gy", "gz"), route)

    def exchange(blocks, routes):
        up, near, mid = blocks
        got = []
        for block, route in zip((near, up, mid), routes):
            got.append(send(block, route))
        return got

    def swap(block):
        return lax.ppermute(block, "gx", [(i, i ^ 1) for i in range(n)])

    (mine,) = call(planes_kernel, (64,), quant_codes)
    other = swap(mine)
    full, faces, scale = pl.pallas_call(
        block_kernel,
        in_specs=[smem, vmem],
        out_shape=(
            shape(quant_codes.shape, I32),
            shape((128, 128), I32),
            shape((8, 128), jnp.float32),
        ),
        compiler_params=params(),
        cost_estimate=pl.CostEstimate(flops=4_000_000, bytes_accessed=1_100_000, transcendentals=0),
        name="block",
    )(error_step, quant_codes)
    (sent,) = call(chip_kernel, (64,), mine, other)
    got = send(sent, across[0])
    sent, state = call(pair_kernel, (64, 64), sent, got, scale)
    got = send(sent, across[1])
    inner = pl.pallas_call(
        functools.partial(inner_kernel, ny=ny, nz=nz),
        out_shape=shape(quant_codes.shape, I32),
        scratch_shapes=[pltpu.VMEM((32, 48, 128), I32)],
        compiler_params=params(),
        cost_estimate=pl.CostEstimate(flops=4_000_000, bytes_accessed=1_100_000, transcendentals=0),
        name="inner",
    )(full, state)
    sent, state = call(quad_kernel, (32, 64), sent, got, state, other, inner)
    their_faces = swap(faces)
    got = send(sent, across[2])
    *sent, z_base, planes = call(
        faces_kernel, (72, 72, 72, 64, 96), got, state, other, faces, their_faces
    )
    got = exchange(sent, along_y)
    rows, *sent = call(columns_kernel, (144, 40, 40, 40), *got, z_base)
    got = exchange(sent, along_z)
    south, north = call(split_kernel, (176, 176), *got, rows, planes)
    pack = swap(south)
    sizes = dict(n=n, ny=ny, nz=nz)
    options = dict(
        out_specs=hbm,
        out_shape=shape(quant_codes.shape, jnp.float32),
        scratch_shapes=[
            pltpu.VMEM(quant_codes.shape, jnp.float32),
            pltpu.SemaphoreType.DMA((4,)),
        ],
        compiler_params=params(),
        cost_estimate=pl.CostEstimate(flops=4_000_000, bytes_accessed=1_100_000, transcendentals=0),
    )
    result = pl.pallas_call(
        functools.partial(north_kernel, **sizes), in_specs=[vmem] * 5, name="north", **options
    )(scale, north, inner, full, planes)
    return pl.pallas_call(
        functools.partial(south_kernel, **sizes),
        in_specs=[vmem] * 5 + [hbm],
        input_output_aliases={5: 0},
        name="south",
        **options,
    )(scale, pack, inner, full, other, result)


def solution(mesh):
    spec = P("gx", "gy", "gz")
    return jax.shard_map(
        on_device, mesh=mesh, in_specs=(spec, P()), out_specs=spec, check_vma=False
    )
```

```python
import functools

import jax
import jax.numpy as jnp
from jax import lax
from jax.experimental import pallas as pl
from jax.experimental.pallas import tpu as pltpu
from jax.sharding import PartitionSpec as P


I32 = jnp.int32
LIMIT = 16 * 1024 * 1024


def params():
    return pltpu.CompilerParams(vmem_limit_bytes=LIMIT)


def at_lane(tile, lane):
    return jnp.broadcast_to(tile[:, lane : lane + 1], tile.shape)


def prefix_lanes(v):
    k = lax.broadcasted_iota(I32, (256, 128), 0)
    upto = (k & 127) <= lax.broadcasted_iota(I32, (256, 128), 1)
    ones = jnp.where(upto, jnp.where(k < 128, 1.0, 256.0), 0.0).astype(jnp.bfloat16)

    def halves(low, high):
        both = jnp.concatenate([low, high], 1).astype(jnp.float32).astype(jnp.bfloat16)
        return jnp.dot(both, ones, preferred_element_type=jnp.float32).astype(I32)

    small = halves(v & 255, (v >> 8) & 255)
    large = halves((v >> 16) & 255, v >> 24)
    return small + (large << 16)


def prefix_planes(v):
    v = prefix_lanes(v).reshape(-1, 8, 128)
    row = lax.broadcasted_iota(I32, v.shape, 1)
    for s in (1, 2, 4):
        v = v + jnp.where(row >= s, pltpu.roll(v, s, 1), 0)
    v = v.reshape(-1, 4, 8, 128)
    tiles = [v[:, 0]]
    for t in range(1, 4):
        tiles.append(v[:, t] + tiles[-1][:, 7:8, :])
    return tiles


def planes_kernel(q, pair):
    sums = [q[i] for i in range(4)]
    for i in range(4, q.shape[0]):
        sums[i % 4] = sums[i % 4] + q[i]
    total = (sums[0] + sums[1]) + (sums[2] + sums[3])
    tiles = prefix_planes(jnp.concatenate([total, q[0]], 0))
    for t in range(4):
        for p in range(2):
            pair[32 * p + 8 * t : 32 * p + 8 * t + 8, :] = tiles[t][p]


def block_kernel(step, q, full, faces, scale):
    nx = q.shape[0]
    lane = lax.broadcasted_iota(I32, (8, 128), 1)
    zero = jnp.zeros((8, 128), I32)
    sums, zl, zf = [zero] * 4, [zero] * 4, [zero] * 4
    for g in range(0, nx, 8):
        tiles = prefix_planes(q[g : g + 8].reshape(256, 128))
        for i in range(8):
            for t in range(4):
                sums[t] = sums[t] + tiles[t][i]
                full[g + i, 8 * t : 8 * t + 8, :] = sums[t]
                zl[t] = jnp.where(lane == g + i, at_lane(sums[t], 127), zl[t])
                zf[t] = jnp.where(lane == g + i, at_lane(sums[t], 0), zf[t])
            faces[g + i : g + i + 1, :] = sums[3][7:8, :]
            faces[32 + g + i : 33 + g + i, :] = sums[0][0:1, :]
    for t in range(4):
        faces[64 + 8 * t : 72 + 8 * t, :] = zl[t]
        faces[96 + 8 * t : 104 + 8 * t, :] = zf[t]
    scale[...] = jnp.full((8, 128), step[0], jnp.float32)


def chip_kernel(mine, other, send):
    send[0:32, :] = mine[0:32, :] + other[0:32, :]
    send[32:64, :] = other[32:64, :]


def pair_kernel(sent, got, _, send, state):
    chip = lax.axis_index("gx") // 2
    odd = chip % 2 == 1
    send[0:32, :] = sent[0:32, :] + got[0:32, :]
    send[32:64, :] = got[32:64, :]
    state[0:32, :] = jnp.where(odd, got[0:32, :], 0)
    state[32:64, :] = got[32:64, :]


def quad_kernel(sent, got, before, other, _, send, state):
    chip = lax.axis_index("gx") // 2
    send[...] = jnp.where(chip == 4, other[32:64, :], sent[0:32, :] + got[0:32, :])
    state[0:32, :] = before[0:32, :] + jnp.where(chip % 4 >= 2, got[0:32, :], 0)
    state[32:64, :] = jnp.where(chip % 4 == 1, got[32:64, :], before[32:64, :])


def faces_kernel(got, before, other, mine, theirs, up, near, mid, z_base, planes):
    chip, y = lax.axis_index("gx") // 2, lax.axis_index("gy")
    lane = lax.broadcasted_iota(I32, (32, 128), 1)
    row = lax.broadcasted_iota(I32, (8, 128), 0)
    c = before[0:32, :] + jnp.where(chip >= 4, got[...], 0)
    nxt = jnp.where(chip == 3, got[...], before[32:64, :])
    d = c + other[0:32, :]
    planes[0:32, :] = c
    planes[32:64, :] = d
    planes[64:96, :] = nxt
    last = d[31:32, :] + mine[31:32, :] + nxt[31:32, :]
    tail = jnp.where(row == 0, c[31:32, :], jnp.where(row == 1, last, 0))
    halves = (theirs, c), (mine, d)
    for k, (face, plane) in enumerate(halves):
        rows = slice(32 * k, 32 * k + 32)
        last_row = face[0:32, :] + plane[31:32, :]
        first_row = face[32:64, :] + plane[0:1, :]
        up[rows, :] = last_row
        near[rows, :] = jnp.where(y % 2 == 1, first_row, last_row)
        mid[rows, :] = jnp.where(y == 2, first_row, last_row)
    for ref in (up, near, mid):
        ref[64:72, :] = tail
    for k, at in ((64, 127), (96, 0)):
        low, high = at_lane(c, at), at_lane(d, at)
        above = high + at_lane(mine[k : k + 32, :], 31) + at_lane(nxt, at)
        base = jnp.where(lane < 32, theirs[k : k + 32, :] + low, 0)
        base = jnp.where((lane >= 32) & (lane < 64), pltpu.roll(mine[k : k + 32, :], 32, 1) + high, base)
        base = jnp.where(lane == 64, low, jnp.where(lane == 65, above, base))
        z_base[k - 64 : k - 32, :] = base


def lower(index, got1, got2, got3):
    one = jnp.where(index % 2 == 1, got1[...], 0)
    two = jnp.where(index >= 2, got2[...], 0)
    return one + two + jnp.where(index >= 2, got3[...], 0)


def beyond(index, got1, got3):
    return jnp.where(index % 2 == 0, got1[...], got3[...])


def columns_kernel(got1, got2, got3, z_base, rows, up, near, mid):
    y, z = lax.axis_index("gy"), lax.axis_index("gz")
    ay = lower(y, got1, got2, got3)
    hy = jnp.where(y < 3, beyond(y, got1, got3), 0)
    rows[0:72, :] = ay
    rows[72:144, :] = hy
    pad = jnp.zeros((56, 128), I32)
    ay_t = jnp.concatenate([ay, pad], 0).T
    hy_t = jnp.concatenate([hy, pad], 0).T
    row = lax.broadcasted_iota(I32, (8, 128), 0)
    end = ay_t[127:128, :]
    tail = jnp.where(row == 0, end, jnp.where(row == 1, hy_t[127:128, :], 0))
    last = z_base[0:32, :] + end
    first = z_base[32:64, :] + ay_t[0:1, :]
    up[0:32, :] = last
    near[0:32, :] = jnp.where(z % 2 == 1, first, last)
    mid[0:32, :] = jnp.where(z == 2, first, last)
    for ref in (up, near, mid):
        ref[32:40, :] = tail


def split_kernel(got1, got2, got3, rows, planes, south, north):
    z = lax.axis_index("gz")
    az = lower(z, got1, got2, got3)
    hz = beyond(z, got1, got3)[0:32, :]
    lane = lax.broadcasted_iota(I32, (40, 128), 1)
    row = lax.broadcasted_iota(I32, (8, 128), 0)

    def tail(a, b):
        return jnp.where(row == 0, rows[a : a + 1, :], jnp.where(row == 1, rows[b : b + 1, :], 0))

    south[0:32, :] = rows[0:32, :]
    south[32:40, :] = tail(64, 32)
    edges = jnp.where(lane == 32, at_lane(az, 64), jnp.where(lane == 33, at_lane(az, 32), az))
    south[40:80, :] = edges
    south[80:112, :] = hz
    south[112:144, :] = rows[72:104, :]
    south[144:176, :] = planes[0:32, :]
    north[0:32, :] = rows[32:64, :]
    north[32:40, :] = tail(31, 65)
    north[40:80, :] = jnp.where(lane == 32, at_lane(az, 31), pltpu.roll(az, 96, 1))
    north[80:112, :] = pltpu.roll(hz, 96, 1)
    north[112:144, :] = rows[104:136, :]
    north[144:176, :] = planes[32:64, :]


def inner_kernel(full, _, inner, field, *, ny, nz):
    has_y = lax.axis_index("gy") < ny - 1
    has_z = lax.axis_index("gz") < nz - 1
    nx = full.shape[0]
    lane = lax.broadcasted_iota(I32, (32, 128), 1)
    for i in range(nx):
        field[i, 8:40, :] = full[i]
        field[i, 7:8, :] = jnp.zeros((1, 128), I32)
        field[i, 40:41, :] = jnp.where(has_y, full[i, 31:32, :], 0)
    for i in range(nx):
        now = full[i]
        total = 6 * now + (field[i, 7:39, :] + field[i, 9:41, :])
        if i > 0:
            total = total + full[i - 1]
        if i < nx - 1:
            total = total + full[i + 1]
        total = total + jnp.where(lane == 0, 0, pltpu.roll(now, 1, 1))
        beyond_z = jnp.where(has_z, now, 0)
        inner[i] = total + jnp.where(lane == 127, beyond_z, pltpu.roll(now, 127, 1))


def stencil(step, pack, inner, full, high, result, out, sems, *, n, ny, nz):
    has_x = lax.axis_index("gx") < n - 1
    has_y = lax.axis_index("gy") < ny - 1
    has_z = lax.axis_index("gz") < nz - 1
    nx = full.shape[0]
    lane = lax.broadcasted_iota(I32, (32, 128), 1)
    row = lax.broadcasted_iota(I32, (32, 128), 0)
    ay, az, hz, hy = pack[0:32, :], pack[40:72, :], pack[80:112, :], pack[112:144, :]
    hyz, low = pack[73:74, :], pack[144:176, :]

    def beside(v, before, after, axis, last):
        at = lane if axis else row
        down = jnp.where(at == 0, before, pltpu.roll(v, 1, axis))
        return down + jnp.where(at == last, after, pltpu.roll(v, (-1) % v.shape[axis], axis))

    def held(flag, v):
        return jnp.where(flag, v, 0)

    rows = 8 * ay + beside(ay, pack[32:33, :], held(has_x, pack[33:34, :]), 0, 31)
    rows = rows + beside(ay, 0, held(has_z, ay), 1, 127)
    cols = 8 * az + beside(az, at_lane(az, 32), held(has_x, at_lane(az, 33)), 1, 31)
    cols = cols + beside(az, pack[72:73, :], held(has_y, az), 0, 31)
    both = 8 * low + beside(low, 0, held(has_y, low), 0, 31)
    both = both + beside(low, 0, held(has_z, low), 1, 127)
    end_y = jnp.where(has_y, hy, -ay)
    hyz = held(has_y, hyz)
    end_z = jnp.where(has_z, hz, -az)
    scale = jnp.broadcast_to(step[0:1, :], (32, 128)) * (1.0 / 12.0)
    ends = jnp.where(lane < 64, cols, pltpu.roll(cols + end_z, 64, 1))
    copies = []
    for i in range(nx):
        picked = jnp.take_along_axis(ends, jnp.where(lane == 127, 64 + i, i), axis=1)
        total = inner[i] + (both + rows[i : i + 1, :]) + picked
        edge = end_y[i : i + 1, :] + jnp.broadcast_to(hyz[:, i : i + 1], (1, 128))
        total = total + jnp.where(row == 31, edge, 0)
        if i == nx - 1:
            total = total + jnp.where(has_x, full[i] + high, -low)
        out[i] = total.astype(jnp.float32) * scale
        if i % 4 == 3:
            part = slice(i - 3, i + 1)
            copies.append(pltpu.make_async_copy(out.at[part], result.at[part], sems.at[i // 4]))
            copies[-1].start()
    for c in copies:
        c.wait()


def north_kernel(step, pack, inner, full, planes, *rest, **sizes):
    @pl.when(lax.axis_index("gx") % 2 == 1)
    def _():
        stencil(step, pack, inner, full, planes[64:96, :], *rest, **sizes)


def south_kernel(step, pack, inner, full, other, _, *rest, **sizes):
    @pl.when(lax.axis_index("gx") % 2 == 0)
    def _():
        stencil(step, pack, inner, full, other[32:64, :], *rest, **sizes)


def routes(n, ny, nz):
    def route(move, south=lambda x, y, z: (x, y ^ 1, z)):
        pairs = []
        for x in range(n):
            for y in range(ny):
                for z in range(nz):
                    to = (move if x % 2 else south)(x, y, z)
                    pairs.append(((x * ny + y) * nz + z, (to[0] * ny + to[1]) * nz + to[2]))
        return pairs

    across = [route(lambda x, y, z, d=d: (x ^ d, y, z)) for d in (2, 4)]
    across.append(route(lambda x, y, z: (n - x, y, z)))

    def middle(x, at, size):
        half = size // 2
        if x % 2:
            return (x, at + half) if at < half else (x - 1, at)
        return (x + 1, at) if at < half else (x, size - 1 - at)

    def far(x, at, size):
        if x % 2:
            return (x, size - 1 - at) if at < size - 1 else (x - 1, at)
        return (x, at - 1) if at else (x + 1, at)

    def in_y(step):
        def move(x, y, z):
            x, y = step(x, y, ny)
            return x, y, z

        return route(move, move)

    def in_z(step):
        def move(x, y, z):
            x, z = step(x, z, nz)
            return x, y, z

        return route(move, move)

    near_y = route(lambda x, y, z: (x, y ^ 1, z))
    near_z = route(lambda x, y, z: (x, y, z ^ 1))
    along_y = [near_y, in_y(middle), in_y(far)]
    along_z = [near_z, in_z(middle), in_z(far)]
    return across, along_y, along_z


def on_device(quant_codes, error_step):
    n, ny, nz = (lax.axis_size(a) for a in ("gx", "gy", "gz"))
    shape = jax.ShapeDtypeStruct
    vmem = pl.BlockSpec(memory_space=pltpu.VMEM)
    smem = pl.BlockSpec(memory_space=pltpu.SMEM)
    hbm = pl.BlockSpec(memory_space=pltpu.HBM)
    across, along_y, along_z = routes(n, ny, nz)

    def call(kernel, rows, *operands, **options):
        outs = tuple(shape((r, 128), I32) for r in rows)
        return pl.pallas_call(
            kernel, out_shape=outs, compiler_params=params(), **options
        )(*operands)

    def send(block, route):
        return lax.ppermute(block, ("gx", "gy", "gz"), route)

    def exchange(blocks, routes):
        up, near, mid = blocks
        got = []
        for block, route in zip((near, up, mid), routes):
            got.append(send(block, route))
        return got

    def swap(block):
        return lax.ppermute(block, "gx", [(i, i ^ 1) for i in range(n)])

    (mine,) = call(planes_kernel, (64,), quant_codes)
    other = swap(mine)
    full, faces, scale = pl.pallas_call(
        block_kernel,
        in_specs=[smem, vmem],
        out_shape=(
            shape(quant_codes.shape, I32),
            shape((128, 128), I32),
            shape((8, 128), jnp.float32),
        ),
        compiler_params=params(),
        cost_estimate=pl.CostEstimate(flops=4_000_000, bytes_accessed=1_100_000, transcendentals=0),
        name="block",
    )(error_step, quant_codes)
    (sent,) = call(chip_kernel, (64,), mine, other)
    got = send(sent, across[0])
    sent, state = call(pair_kernel, (64, 64), sent, got, scale)
    got = send(sent, across[1])
    inner = pl.pallas_call(
        functools.partial(inner_kernel, ny=ny, nz=nz),
        out_shape=shape(quant_codes.shape, I32),
        scratch_shapes=[pltpu.VMEM((32, 48, 128), I32)],
        compiler_params=params(),
        cost_estimate=pl.CostEstimate(flops=4_000_000, bytes_accessed=1_100_000, transcendentals=0),
        name="inner",
    )(full, state)
    sent, state = call(quad_kernel, (32, 64), sent, got, state, other, inner)
    their_faces = swap(faces)
    got = send(sent, across[2])
    *sent, z_base, planes = call(
        faces_kernel, (72, 72, 72, 64, 96), got, state, other, faces, their_faces
    )
    got = exchange(sent, along_y)
    rows, *sent = call(columns_kernel, (144, 40, 40, 40), *got, z_base)
    got = exchange(sent, along_z)
    south, north = call(split_kernel, (176, 176), *got, rows, planes)
    pack = swap(south)
    sizes = dict(n=n, ny=ny, nz=nz)
    options = dict(
        out_specs=hbm,
        out_shape=shape(quant_codes.shape, jnp.float32),
        scratch_shapes=[
            pltpu.VMEM(quant_codes.shape, jnp.float32),
            pltpu.SemaphoreType.DMA((8,)),
        ],
        compiler_params=params(),
        cost_estimate=pl.CostEstimate(flops=4_000_000, bytes_accessed=1_100_000, transcendentals=0),
    )
    result = pl.pallas_call(
        functools.partial(north_kernel, **sizes), in_specs=[vmem] * 5, name="north", **options
    )(scale, north, inner, full, planes)
    return pl.pallas_call(
        functools.partial(south_kernel, **sizes),
        in_specs=[vmem] * 5 + [hbm],
        input_output_aliases={5: 0},
        name="south",
        **options,
    )(scale, pack, inner, full, other, result)


def solution(mesh):
    spec = P("gx", "gy", "gz")
    return jax.shard_map(
        on_device, mesh=mesh, in_specs=(spec, P()), out_specs=spec, check_vma=False
    )
```

```python
import functools

import jax
import jax.numpy as jnp
from jax import lax
from jax.experimental import pallas as pl
from jax.experimental.pallas import tpu as pltpu
from jax.sharding import PartitionSpec as P


I32 = jnp.int32
LIMIT = 16 * 1024 * 1024


def params():
    return pltpu.CompilerParams(vmem_limit_bytes=LIMIT)


def at_lane(tile, lane):
    return jnp.broadcast_to(tile[:, lane : lane + 1], tile.shape)


def prefix_lanes(v):
    k = lax.broadcasted_iota(I32, (256, 128), 0)
    upto = (k & 127) <= lax.broadcasted_iota(I32, (256, 128), 1)
    ones = jnp.where(upto, jnp.where(k < 128, 1.0, 256.0), 0.0).astype(jnp.bfloat16)

    def halves(low, high):
        both = jnp.concatenate([low, high], 1).astype(jnp.float32).astype(jnp.bfloat16)
        return jnp.dot(both, ones, preferred_element_type=jnp.float32).astype(I32)

    small = halves(v & 255, (v >> 8) & 255)
    large = halves((v >> 16) & 255, v >> 24)
    return small + (large << 16)


def prefix_planes(v):
    v = prefix_lanes(v).reshape(-1, 8, 128)
    row = lax.broadcasted_iota(I32, v.shape, 1)
    for s in (1, 2, 4):
        v = v + jnp.where(row >= s, pltpu.roll(v, s, 1), 0)
    v = v.reshape(-1, 4, 8, 128)
    tiles = [v[:, 0]]
    for t in range(1, 4):
        tiles.append(v[:, t] + tiles[-1][:, 7:8, :])
    return tiles


def planes_kernel(q, pair):
    sums = [q[i] for i in range(4)]
    for i in range(4, q.shape[0]):
        sums[i % 4] = sums[i % 4] + q[i]
    total = (sums[0] + sums[1]) + (sums[2] + sums[3])
    tiles = prefix_planes(jnp.concatenate([total, q[0]], 0))
    for t in range(4):
        for p in range(2):
            pair[32 * p + 8 * t : 32 * p + 8 * t + 8, :] = tiles[t][p]


def block_kernel(step, q, full, faces, scale):
    nx = q.shape[0]
    lane = lax.broadcasted_iota(I32, (8, 128), 1)
    zero = jnp.zeros((8, 128), I32)
    sums, zl, zf = [zero] * 4, [zero] * 4, [zero] * 4
    for g in range(0, nx, 8):
        tiles = prefix_planes(q[g : g + 8].reshape(256, 128))
        for i in range(8):
            for t in range(4):
                sums[t] = sums[t] + tiles[t][i]
                full[g + i, 8 * t : 8 * t + 8, :] = sums[t]
                zl[t] = jnp.where(lane == g + i, at_lane(sums[t], 127), zl[t])
                zf[t] = jnp.where(lane == g + i, at_lane(sums[t], 0), zf[t])
            faces[g + i : g + i + 1, :] = sums[3][7:8, :]
            faces[32 + g + i : 33 + g + i, :] = sums[0][0:1, :]
    for t in range(4):
        faces[64 + 8 * t : 72 + 8 * t, :] = zl[t]
        faces[96 + 8 * t : 104 + 8 * t, :] = zf[t]
    scale[...] = jnp.full((8, 128), step[0], jnp.float32)


def chip_kernel(mine, other, send):
    send[0:32, :] = mine[0:32, :] + other[0:32, :]
    send[32:64, :] = other[32:64, :]


def pair_kernel(sent, got, _, send, state):
    chip = lax.axis_index("gx") // 2
    odd = chip % 2 == 1
    send[0:32, :] = sent[0:32, :] + got[0:32, :]
    send[32:64, :] = got[32:64, :]
    state[0:32, :] = jnp.where(odd, got[0:32, :], 0)
    state[32:64, :] = got[32:64, :]


def quad_kernel(sent, got, before, other, _, send, state):
    chip = lax.axis_index("gx") // 2
    send[...] = jnp.where(chip == 4, other[32:64, :], sent[0:32, :] + got[0:32, :])
    state[0:32, :] = before[0:32, :] + jnp.where(chip % 4 >= 2, got[0:32, :], 0)
    state[32:64, :] = jnp.where(chip % 4 == 1, got[32:64, :], before[32:64, :])


def faces_kernel(got, before, other, mine, theirs, up, near, mid, z_base, planes):
    chip, y = lax.axis_index("gx") // 2, lax.axis_index("gy")
    lane = lax.broadcasted_iota(I32, (32, 128), 1)
    row = lax.broadcasted_iota(I32, (8, 128), 0)
    c = before[0:32, :] + jnp.where(chip >= 4, got[...], 0)
    nxt = jnp.where(chip == 3, got[...], before[32:64, :])
    d = c + other[0:32, :]
    planes[0:32, :] = c
    planes[32:64, :] = d
    planes[64:96, :] = nxt
    last = d[31:32, :] + mine[31:32, :] + nxt[31:32, :]
    tail = jnp.where(row == 0, c[31:32, :], jnp.where(row == 1, last, 0))
    halves = (theirs, c), (mine, d)
    for k, (face, plane) in enumerate(halves):
        rows = slice(32 * k, 32 * k + 32)
        last_row = face[0:32, :] + plane[31:32, :]
        first_row = face[32:64, :] + plane[0:1, :]
        up[rows, :] = last_row
        near[rows, :] = jnp.where(y % 2 == 1, first_row, last_row)
        mid[rows, :] = jnp.where(y == 2, first_row, last_row)
    for ref in (up, near, mid):
        ref[64:72, :] = tail
    for k, at in ((64, 127), (96, 0)):
        low, high = at_lane(c, at), at_lane(d, at)
        above = high + at_lane(mine[k : k + 32, :], 31) + at_lane(nxt, at)
        base = jnp.where(lane < 32, theirs[k : k + 32, :] + low, 0)
        base = jnp.where((lane >= 32) & (lane < 64), pltpu.roll(mine[k : k + 32, :], 32, 1) + high, base)
        base = jnp.where(lane == 64, low, jnp.where(lane == 65, above, base))
        z_base[k - 64 : k - 32, :] = base


def lower(index, got1, got2, got3):
    one = jnp.where(index % 2 == 1, got1[...], 0)
    two = jnp.where(index >= 2, got2[...], 0)
    return one + two + jnp.where(index >= 2, got3[...], 0)


def beyond(index, got1, got3):
    return jnp.where(index % 2 == 0, got1[...], got3[...])


def columns_kernel(got1, got2, got3, z_base, rows, up, near, mid):
    y, z = lax.axis_index("gy"), lax.axis_index("gz")
    ay = lower(y, got1, got2, got3)
    hy = jnp.where(y < 3, beyond(y, got1, got3), 0)
    rows[0:72, :] = ay
    rows[72:144, :] = hy
    pad = jnp.zeros((56, 128), I32)
    ay_t = jnp.concatenate([ay, pad], 0).T
    hy_t = jnp.concatenate([hy, pad], 0).T
    row = lax.broadcasted_iota(I32, (8, 128), 0)
    end = ay_t[127:128, :]
    tail = jnp.where(row == 0, end, jnp.where(row == 1, hy_t[127:128, :], 0))
    last = z_base[0:32, :] + end
    first = z_base[32:64, :] + ay_t[0:1, :]
    up[0:32, :] = last
    near[0:32, :] = jnp.where(z % 2 == 1, first, last)
    mid[0:32, :] = jnp.where(z == 2, first, last)
    for ref in (up, near, mid):
        ref[32:40, :] = tail


def split_kernel(got1, got2, got3, rows, planes, south, north):
    z = lax.axis_index("gz")
    az = lower(z, got1, got2, got3)
    hz = pltpu.roll(beyond(z, got1, got3), 64, 1)
    lane = lax.broadcasted_iota(I32, (40, 128), 1)
    row = lax.broadcasted_iota(I32, (8, 128), 0)

    def tail(a, b):
        return jnp.where(row == 0, rows[a : a + 1, :], jnp.where(row == 1, rows[b : b + 1, :], 0))

    south[0:32, :] = rows[0:32, :]
    south[32:40, :] = tail(64, 32)
    edges = jnp.where(lane == 32, at_lane(az, 64), jnp.where(lane == 33, at_lane(az, 32), az))
    south[40:80, :] = jnp.where(lane < 64, edges, hz)
    south[80:112, :] = rows[72:104, :]
    south[112:144, :] = planes[0:32, :]
    north[0:32, :] = rows[32:64, :]
    north[32:40, :] = tail(31, 65)
    edges = jnp.where(lane == 32, at_lane(az, 31), pltpu.roll(az, 96, 1))
    north[40:80, :] = jnp.where(lane < 64, edges, pltpu.roll(hz, 96, 1))
    north[80:112, :] = rows[104:136, :]
    north[112:144, :] = planes[32:64, :]


def inner_kernel(full, _, inner, field, *, ny, nz):
    has_y = lax.axis_index("gy") < ny - 1
    has_z = lax.axis_index("gz") < nz - 1
    nx = full.shape[0]
    lane = lax.broadcasted_iota(I32, (32, 128), 1)
    for i in range(nx):
        field[i, 8:40, :] = full[i]
        field[i, 7:8, :] = jnp.zeros((1, 128), I32)
        field[i, 40:41, :] = jnp.where(has_y, full[i, 31:32, :], 0)
    for i in range(nx):
        now = full[i]
        total = 6 * now + (field[i, 7:39, :] + field[i, 9:41, :])
        if i > 0:
            total = total + full[i - 1]
        if i < nx - 1:
            total = total + full[i + 1]
        total = total + jnp.where(lane == 0, 0, pltpu.roll(now, 1, 1))
        beyond_z = jnp.where(has_z, now, 0)
        inner[i] = total + jnp.where(lane == 127, beyond_z, pltpu.roll(now, 127, 1))


def stencil(step, pack, inner, full, high, result, out, sems, *, n, ny, nz):
    has_x = lax.axis_index("gx") < n - 1
    has_y = lax.axis_index("gy") < ny - 1
    has_z = lax.axis_index("gz") < nz - 1
    nx = full.shape[0]
    lane = lax.broadcasted_iota(I32, (32, 128), 1)
    row = lax.broadcasted_iota(I32, (32, 128), 0)
    ay, az, hy = pack[0:32, :], pack[40:72, :], pack[80:112, :]
    hz = pltpu.roll(az, 64, 1)
    hyz, low = pack[73:74, :], pack[112:144, :]

    def beside(v, before, after, axis, last):
        at = lane if axis else row
        down = jnp.where(at == 0, before, pltpu.roll(v, 1, axis))
        return down + jnp.where(at == last, after, pltpu.roll(v, (-1) % v.shape[axis], axis))

    def held(flag, v):
        return jnp.where(flag, v, 0)

    rows = 8 * ay + beside(ay, pack[32:33, :], held(has_x, pack[33:34, :]), 0, 31)
    rows = rows + beside(ay, 0, held(has_z, ay), 1, 127)
    cols = 8 * az + beside(az, at_lane(az, 32), held(has_x, at_lane(az, 33)), 1, 31)
    cols = cols + beside(az, pack[72:73, :], held(has_y, az), 0, 31)
    both = 8 * low + beside(low, 0, held(has_y, low), 0, 31)
    both = both + beside(low, 0, held(has_z, low), 1, 127)
    end_y = jnp.where(has_y, hy, -ay)
    hyz = held(has_y, hyz)
    end_z = jnp.where(has_z, hz, -az)
    scale = jnp.broadcast_to(step[0:1, :], (32, 128)) * (1.0 / 12.0)
    ends = jnp.where(lane < 64, cols, pltpu.roll(cols + end_z, 64, 1))
    copies = []
    for i in range(nx):
        picked = jnp.take_along_axis(ends, jnp.where(lane == 127, 64 + i, i), axis=1)
        total = inner[i] + (both + rows[i : i + 1, :]) + picked
        edge = end_y[i : i + 1, :] + jnp.broadcast_to(hyz[:, i : i + 1], (1, 128))
        total = total + jnp.where(row == 31, edge, 0)
        if i == nx - 1:
            total = total + jnp.where(has_x, full[i] + high, -low)
        out[i] = total.astype(jnp.float32) * scale
        if i % 4 == 3:
            part = slice(i - 3, i + 1)
            copies.append(pltpu.make_async_copy(out.at[part], result.at[part], sems.at[i // 4]))
            copies[-1].start()
    for c in copies:
        c.wait()


def north_kernel(step, pack, inner, full, planes, *rest, **sizes):
    @pl.when(lax.axis_index("gx") % 2 == 1)
    def _():
        stencil(step, pack, inner, full, planes[64:96, :], *rest, **sizes)


def south_kernel(step, pack, inner, full, other, _, *rest, **sizes):
    @pl.when(lax.axis_index("gx") % 2 == 0)
    def _():
        stencil(step, pack, inner, full, other[32:64, :], *rest, **sizes)


def routes(n, ny, nz):
    def route(move, south=lambda x, y, z: (x, y ^ 1, z)):
        pairs = []
        for x in range(n):
            for y in range(ny):
                for z in range(nz):
                    to = (move if x % 2 else south)(x, y, z)
                    pairs.append(((x * ny + y) * nz + z, (to[0] * ny + to[1]) * nz + to[2]))
        return pairs

    across = [route(lambda x, y, z, d=d: (x ^ d, y, z)) for d in (2, 4)]
    across.append(route(lambda x, y, z: (n - x, y, z)))

    def middle(x, at, size):
        half = size // 2
        if x % 2:
            return (x, at + half) if at < half else (x - 1, at)
        return (x + 1, at) if at < half else (x, size - 1 - at)

    def far(x, at, size):
        if x % 2:
            return (x, size - 1 - at) if at < size - 1 else (x - 1, at)
        return (x, at - 1) if at else (x + 1, at)

    def in_y(step):
        def move(x, y, z):
            x, y = step(x, y, ny)
            return x, y, z

        return route(move, move)

    def in_z(step):
        def move(x, y, z):
            x, z = step(x, z, nz)
            return x, y, z

        return route(move, move)

    near_y = route(lambda x, y, z: (x, y ^ 1, z))
    near_z = route(lambda x, y, z: (x, y, z ^ 1))
    along_y = [near_y, in_y(middle), in_y(far)]
    along_z = [near_z, in_z(middle), in_z(far)]
    return across, along_y, along_z


def on_device(quant_codes, error_step):
    n, ny, nz = (lax.axis_size(a) for a in ("gx", "gy", "gz"))
    shape = jax.ShapeDtypeStruct
    vmem = pl.BlockSpec(memory_space=pltpu.VMEM)
    smem = pl.BlockSpec(memory_space=pltpu.SMEM)
    hbm = pl.BlockSpec(memory_space=pltpu.HBM)
    across, along_y, along_z = routes(n, ny, nz)

    def call(kernel, rows, *operands, **options):
        outs = tuple(shape((r, 128), I32) for r in rows)
        return pl.pallas_call(
            kernel, out_shape=outs, compiler_params=params(), **options
        )(*operands)

    def send(block, route):
        return lax.ppermute(block, ("gx", "gy", "gz"), route)

    def exchange(blocks, routes):
        up, near, mid = blocks
        got = []
        for block, route in zip((near, up, mid), routes):
            got.append(send(block, route))
        return got

    def swap(block):
        return lax.ppermute(block, "gx", [(i, i ^ 1) for i in range(n)])

    (mine,) = call(planes_kernel, (64,), quant_codes)
    other = swap(mine)
    full, faces, scale = pl.pallas_call(
        block_kernel,
        in_specs=[smem, vmem],
        out_shape=(
            shape(quant_codes.shape, I32),
            shape((128, 128), I32),
            shape((8, 128), jnp.float32),
        ),
        compiler_params=params(),
        cost_estimate=pl.CostEstimate(flops=4_000_000, bytes_accessed=1_100_000, transcendentals=0),
        name="block",
    )(error_step, quant_codes)
    (sent,) = call(chip_kernel, (64,), mine, other)
    got = send(sent, across[0])
    sent, state = call(pair_kernel, (64, 64), sent, got, scale)
    got = send(sent, across[1])
    inner = pl.pallas_call(
        functools.partial(inner_kernel, ny=ny, nz=nz),
        out_shape=shape(quant_codes.shape, I32),
        scratch_shapes=[pltpu.VMEM((32, 48, 128), I32)],
        compiler_params=params(),
        cost_estimate=pl.CostEstimate(flops=4_000_000, bytes_accessed=1_100_000, transcendentals=0),
        name="inner",
    )(full, state)
    sent, state = call(quad_kernel, (32, 64), sent, got, state, other, inner)
    their_faces = swap(faces)
    got = send(sent, across[2])
    *sent, z_base, planes = call(
        faces_kernel, (72, 72, 72, 64, 96), got, state, other, faces, their_faces
    )
    got = exchange(sent, along_y)
    rows, *sent = call(columns_kernel, (144, 40, 40, 40), *got, z_base)
    got = exchange(sent, along_z)
    south, north = call(split_kernel, (144, 144), *got, rows, planes)
    pack = swap(south)
    sizes = dict(n=n, ny=ny, nz=nz)
    options = dict(
        out_specs=hbm,
        out_shape=shape(quant_codes.shape, jnp.float32),
        scratch_shapes=[
            pltpu.VMEM(quant_codes.shape, jnp.float32),
            pltpu.SemaphoreType.DMA((8,)),
        ],
        compiler_params=params(),
        cost_estimate=pl.CostEstimate(flops=4_000_000, bytes_accessed=1_100_000, transcendentals=0),
    )
    result = pl.pallas_call(
        functools.partial(north_kernel, **sizes), in_specs=[vmem] * 5, name="north", **options
    )(scale, north, inner, full, planes)
    return pl.pallas_call(
        functools.partial(south_kernel, **sizes),
        in_specs=[vmem] * 5 + [hbm],
        input_output_aliases={5: 0},
        name="south",
        **options,
    )(scale, pack, inner, full, other, result)


def solution(mesh):
    spec = P("gx", "gy", "gz")
    return jax.shard_map(
        on_device, mesh=mesh, in_specs=(spec, P()), out_specs=spec, check_vma=False
    )
```
